128 devices in a mesh: req: 2 (over core), seq: 64 (over x, z, y).
Axes of the slice: x: 4, y: 4, z: 4, core: 2. Of those that a mesh axis runs over, the one named last changes fastest.
Arguments:
- image_query: bfloat16 [1024, 1536], P(('req', 'seq')), parts along dimension 0, may hold values from -6 to 6
- image_key: bfloat16 [1024, 1536], P(('req', 'seq')), parts along dimension 0, may hold values from -6 to 6
- image_value: bfloat16 [1024, 1536], P(('req', 'seq')), parts along dimension 0, may hold values from -6 to 6
- text_query: bfloat16 [1024, 1536], P('req'), parts along dimension 0, may hold values from -6 to 6
- text_key: bfloat16 [1024, 1536], P('req'), parts along dimension 0, may hold values from -6 to 6
- text_value: bfloat16 [1024, 1536], P('req'), parts along dimension 0, may hold values from -6 to 6
- image_query_gain: float32 [128], replicated, may hold values from 1 to 8
- image_key_gain: float32 [128], replicated, may hold values from 1 to 8
- text_query_gain: float32 [128], replicated, may hold values from 1 to 2.5
- text_key_gain: float32 [128], replicated, may hold values from 1 to 2.5
- image_order: int32 [1024], P(('req', 'seq')), parts along dimension 0, may hold values from 0 to 511, each once
- text_length: int32 [2], P('req'), parts along dimension 0, may hold values from 256 to 512
Outputs:
- image_out: bfloat16 [1024, 1536], P(('req', 'seq')), parts along dimension 0
- text_out: bfloat16 [1024, 1536], P(('req', 'seq')), parts along dimension 0
The draws below stay inside these ranges and needn't reach their ends.
There are 2 independent parts, one for each index of `req`. The reference program is written for one: setup_inputs(seed, part) draws one part's arguments, and reference() takes and returns one part's arrays. A program takes and returns all parts, laid end to end along the dimension named above; an argument that names none is the same for every part. Nothing has to cross between parts.
Inputs may be any that keep to these rules, and one draw needn't show every extreme that they name: `image_order`: every position 0 to 511 appears once.
All inputs are finite; a program needn't handle non-finite values.
Results may differ from the reference program's by a relative error of at most 0.005.
The reference program's roundings to bfloat16 on the way (of `weights`) count: a program that leaves them out, or rounds other values in their place, can miss the bound.
Values may be sent and summed in bfloat16 or wider, within the bound.
A program may use at most 64 MiB of HBM per device.

```python
import jax
import jax.numpy as jnp
from jax import lax

H = 12
HD = 128
TXT = 512
GRID_W = 64
TOK_DEV = 8
IMG = 512
N_SEQ = 64


def draw_image_query(key, part):
    queries = jax.random.normal(jax.random.fold_in(key, 1), (IMG, H * HD), jnp.float32)
    return jnp.clip(queries, -6.0, 6.0).astype(jnp.bfloat16)


def draw_image_key(key, part):
    keys_drawn = jax.random.normal(jax.random.fold_in(key, 2), (IMG, H * HD), jnp.float32)
    return jnp.clip(keys_drawn, -6.0, 6.0).astype(jnp.bfloat16)


def draw_image_query_gain(key, part):
    return jax.random.uniform(jax.random.fold_in(key, 5), (HD,), jnp.float32, 1.0, 2.5)


def draw_image_key_gain(key, part):
    return jax.random.uniform(jax.random.fold_in(key, 6), (HD,), jnp.float32, 1.0, 2.5)


def level_of(own_key, dims, cuts, low, top_value):
    level, own = 1.0, jax.random.fold_in(own_key, 6)
    for dim, parts in cuts:
        heights = jnp.exp(jax.random.uniform(jax.random.fold_in(own, dim), (parts,), jnp.float32, low / len(cuts), top_value / len(cuts)))
        level = level * jnp.repeat(heights, dims[dim] // parts).reshape([-1 if axis == dim else 1 for axis in range(len(dims))])
    return level


def bell_draw(stream_key, dims, deviation, limit, pieces=(), held_as=jnp.bfloat16):
    level = level_of(stream_key, dims, pieces, -0.22, 0.18) if pieces else 1.0
    values = jax.random.normal(stream_key, dims, jnp.float32) * deviation * level
    return jnp.minimum(jnp.maximum(values, -limit), limit).astype(held_as)


def setup_inputs(seed: int = 0, part: int = 0) -> dict:
    key_of = jax.random.split(jax.random.key(seed), 13)
    part_keys = jax.random.split(jax.random.fold_in(key_of[12], part), 13)
    image_query = draw_image_query(jax.random.fold_in(jax.random.fold_in(key_of[12], part), 71), part)
    image_key = draw_image_key(jax.random.fold_in(jax.random.fold_in(key_of[12], part), 71), part)
    image_value = bell_draw(part_keys[2], (IMG, H * HD), 1.0, 6.0, ((0, 64),))
    text_query = bell_draw(part_keys[3], (TXT, H * HD), 1.0, 6.0)
    text_key = bell_draw(part_keys[4], (TXT, H * HD), 1.0, 6.0)
    text_value = bell_draw(part_keys[5], (TXT, H * HD), 1.0, 6.0)
    image_query_gain = draw_image_query_gain(jax.random.fold_in(key_of[12], 71), part)
    image_key_gain = draw_image_key_gain(jax.random.fold_in(key_of[12], 71), part)
    text_query_gain = jnp.clip(jax.random.uniform(key_of[8], (HD,), jnp.float32, 1.0, 2.5), 1.0, 2.5)
    text_key_gain = jnp.clip(jax.random.uniform(key_of[9], (HD,), jnp.float32, 1.0, 2.5), 1.0, 2.5)
    image_order = jax.random.permutation(part_keys[10], IMG).astype(jnp.int32)
    text_length = jax.random.randint(part_keys[11], (1,), TXT // 2, TXT + 1).astype(jnp.int32)
    return {"image_query": image_query, "image_key": image_key, "image_value": image_value, "text_query": text_query, "text_key": text_key, "text_value": text_value, "image_query_gain": image_query_gain, "image_key_gain": image_key_gain, "text_query_gain": text_query_gain, "text_key_gain": text_key_gain, "image_order": image_order, "text_length": text_length}


epsilon = 1e-06
masked_score = -1e+30

def head_norm(values, norm_gain, head_count):
    row_count = values.shape[0]
    shaped = values.astype(jnp.float32).reshape(row_count, head_count, -1)
    mean_square = lax.optimization_barrier(jnp.mean(shaped * shaped, axis=-1, keepdims=True))
    return shaped * lax.rsqrt(mean_square + epsilon) * norm_gain

def rotate(normed, positions, half_length):
    row_count, head_count, head_dim = normed.shape
    pair_count = head_dim // 2
    pair_ids = jnp.arange(pair_count)
    first_axis = pair_ids < 8
    second = pair_ids < 36
    within = jnp.where(first_axis, pair_ids, jnp.where(second, pair_ids - 8, pair_ids - 36)).astype(jnp.float32)
    axis_dim = jnp.where(first_axis, 16.0, 56.0).astype(jnp.float32)
    frequency = jnp.power(jnp.float32(10000.0), -2.0 * within / axis_dim)
    image_index = positions // half_length
    inside = positions % half_length
    row_place = inside // GRID_W
    column_place = inside % GRID_W
    coordinate = jnp.where(first_axis[None, :], image_index[:, None], jnp.where(second[None, :], row_place[:, None], column_place[:, None])).astype(jnp.float32)
    angles = coordinate * frequency[None, :]
    cosine = jnp.cos(angles)[:, None, :]
    sine_part = jnp.sin(angles)[:, None, :]
    paired = normed.reshape(row_count, head_count, pair_count, 2)
    even_part = paired[..., 0]
    odd_part = paired[..., 1]
    turned = jnp.stack([even_part * cosine - odd_part * sine_part, even_part * sine_part + odd_part * cosine], axis=-1)
    return turned.reshape(row_count, head_count * head_dim)

def reference(image_query, image_key, image_value, text_query, text_key, text_value, image_query_gain, image_key_gain, text_query_gain, text_key_gain, image_order, text_length):
    head_count = image_query.shape[1] // HD
    half_length = IMG // 2
    query_img = lax.optimization_barrier(rotate(head_norm(image_query, image_query_gain, head_count), image_order, half_length).astype(jnp.bfloat16))
    key_img = lax.optimization_barrier(rotate(head_norm(image_key, image_key_gain, head_count), image_order, half_length).astype(jnp.bfloat16))
    query_txt = lax.optimization_barrier(head_norm(text_query, text_query_gain, head_count).reshape(TXT, -1).astype(jnp.bfloat16))
    key_txt = lax.optimization_barrier(head_norm(text_key, text_key_gain, head_count).reshape(TXT, -1).astype(jnp.bfloat16))
    all_keys = jnp.concatenate([key_txt, key_img], axis=0).astype(jnp.float32)
    all_values = jnp.concatenate([text_value, image_value], axis=0).astype(jnp.float32)
    key_count = all_keys.shape[0]
    key_heads = all_keys.reshape(key_count, head_count, HD)
    value_heads = all_values.reshape(key_count, head_count, HD)
    valid = jnp.concatenate([jnp.arange(TXT) < text_length[0], jnp.ones((IMG,), dtype=bool)])
    scaling = HD ** (-0.5)

    def attend(block):
        row_count = block.shape[0]
        query_heads = block.astype(jnp.float32).reshape(row_count, head_count, HD)
        scores = jnp.einsum('rhd,shd->rhs', query_heads, key_heads) * scaling
        scores = jnp.where(valid[None, None, :], scores, masked_score)
        row_max = lax.optimization_barrier(jnp.max(scores, axis=-1))
        expo = jnp.exp(scores - row_max[..., None])
        expo = jnp.where(valid[None, None, :], expo, 0.0)
        totals = lax.optimization_barrier(jnp.sum(expo, axis=-1))
        weights = lax.optimization_barrier(expo.astype(jnp.bfloat16)).astype(jnp.float32)
        blended = jnp.einsum('rhs,shd->rhd', weights, value_heads)
        return (blended / totals[..., None]).reshape(row_count, -1).astype(jnp.bfloat16)
    text_out = lax.map(attend, query_txt.reshape(N_SEQ, TXT // N_SEQ, -1)).reshape(TXT, -1)
    image_out = lax.map(attend, query_img.reshape(N_SEQ, TOK_DEV, -1)).reshape(IMG, -1)
    return (image_out, text_out)
```

```python
import jax
import jax.numpy as jnp
from jax import lax
from jax.experimental import pallas as pl
from jax.experimental.pallas import tpu as pltpu
from jax.sharding import PartitionSpec as P

GRID_W = 64
EPS = 1e-06
NEG = -1e30
MESH = pl.DeviceIdType.MESH
HEADS = 12
HD = 128
ROWS = 8
PLANE = 16
SEQ = 64
LOG2E = 1.4426950408889634

OFFSETS = [(2, 2), (2, 1), (2, 3), (1, 2), (3, 2), (1, 1), (1, 3), (3, 1), (3, 3), (2, 0), (0, 2),
           (1, 0), (3, 0), (0, 1), (0, 3), (0, 0)]


def normed(x, gain):
    mean_square = jnp.mean(x * x, axis=-1, keepdims=True)
    return x * lax.rsqrt(mean_square + EPS) * gain


def rotary(order_ref):
    row = lax.broadcasted_iota(jnp.int32, (ROWS, HD), 0)
    lane = lax.broadcasted_iota(jnp.int32, (ROWS, HD), 1)
    position = jnp.zeros((ROWS, HD), jnp.int32)
    for r in range(ROWS):
        position = jnp.where(row == r, order_ref[r], position)
    pair = lane >> 1
    first = pair < 8
    second = pair < 36
    within = jnp.where(first, pair, jnp.where(second, pair - 8, pair - 36)).astype(jnp.float32)
    width = jnp.where(first, 16.0, 56.0).astype(jnp.float32)
    frequency = jnp.exp(within / width * jnp.float32(-2.0 * 9.210340371976184))
    half = 4 * GRID_W
    inside = position & (half - 1)
    place = jnp.where(first, position >> 8, jnp.where(second, inside >> 6, inside & (GRID_W - 1)))
    angle = place.astype(jnp.float32) * frequency
    even = (lane & 1) == 0
    sine = jnp.sin(angle)
    return jnp.cos(angle), jnp.where(even, -sine, sine), even


def turn(x, cosine, sine, even):
    other = jnp.where(even, pltpu.roll(x, HD - 1, 1), pltpu.roll(x, 1, 1))
    return x * cosine + other * sine


def scores_of(q, k):
    return lax.dot_general(q, k, (((1,), (1,)), ((), ())), preferred_element_type=jnp.float32)


def kernel(order_ref, length_ref, iq_hbm, ik_hbm, iv_hbm, tq_hbm, tk_hbm, tv_hbm, gains_hbm,
           image_out, text_out,
           iq, ik, iv, tq, tk, tv, gains, kv_out, q_out, kv_in, q_in, o_out, o_in,
           load_sem, kv_send, kv_recv, q_send, q_recv, o_send, o_recv):
    me = lax.axis_index("seq")
    x, z, y = me // 16, (me // 4) % 4, me % 4
    spot = me % PLANE
    slot = (y - z + 3) % 4
    owner = slot < 3
    head = z * 3 + jnp.minimum(slot, 2)
    scale = HD ** -0.5 * LOG2E

    barrier = pltpu.get_barrier_semaphore()

    def greet(i, c):
        pl.semaphore_signal(barrier, inc=1, device_id={"seq": (me + i) % SEQ}, device_id_type=MESH)
        return c

    lax.fori_loop(1, SEQ, greet, 0)

    column = pl.ds(pl.multiple_of(head * HD, HD), HD)
    loads = [
        pltpu.make_async_copy(ik_hbm, ik, load_sem.at[0]),
        pltpu.make_async_copy(iv_hbm, iv, load_sem.at[1]),
        pltpu.make_async_copy(iq_hbm, iq, load_sem.at[2]),
        pltpu.make_async_copy(gains_hbm, gains, load_sem.at[3]),
        pltpu.make_async_copy(tk_hbm.at[:, column], tk, load_sem.at[4]),
        pltpu.make_async_copy(
            tq_hbm.at[pl.ds(pl.multiple_of(x * 128, 128), 128), column], tq, load_sem.at[5]),
        pltpu.make_async_copy(tv_hbm.at[:, column], tv, load_sem.at[6]),
    ]
    for load in loads:
        load.start()
    cosine, sine, even = rotary(order_ref)
    for load in loads[:4]:
        load.wait()

    for h in range(HEADS):
        cols = slice(h * HD, (h + 1) * HD)
        k = turn(normed(ik[:, cols].astype(jnp.float32), gains[1:2, :]), cosine, sine, even)
        v = iv[:, cols].astype(jnp.float32)
        kv_out[h] = jnp.concatenate([k, v], axis=0).astype(jnp.bfloat16)
        q = turn(normed(iq[:, cols].astype(jnp.float32), gains[0:1, :]), cosine, sine, even)
        q_out[h] = q.astype(jnp.bfloat16).astype(jnp.float32)

    pl.semaphore_wait(barrier, SEQ - 1)

    js = [(j + y) % 3 for j in range(3)]

    def kv_copy(h, to):
        return pltpu.make_async_remote_copy(
            src_ref=kv_out.at[h], dst_ref=kv_in.at[me], send_sem=kv_send, recv_sem=kv_recv,
            device_id={"seq": to}, device_id_type=MESH)

    def q_copy(h, to):
        return pltpu.make_async_remote_copy(
            src_ref=q_out.at[h], dst_ref=q_in.at[spot], send_sem=q_send, recv_sem=q_recv,
            device_id={"seq": to}, device_id_type=MESH)

    def owners(dx, dz):
        tx, tz = (x + dx) % 4, (z + dz) % 4
        for j in js:
            yield tz * 3 + j, tx * 16 + tz * 4 + (tz + 1 + j) % 4

    for dx, dz in OFFSETS:
        for h, to in owners(dx, dz):
            if dx == 0 and dz == 0:
                @pl.when(to != me)
                def _():
                    kv_copy(h, to).start()
                    q_copy(h, to).start()
            else:
                kv_copy(h, to).start()
                if dx == 0:
                    q_copy(h, to).start()

    @pl.when(owner)
    def _():
        kv_in[me] = kv_out[head]
        q_in[spot] = q_out[head]
        for load in loads[4:]:
            load.wait()
        keys = normed(tk[...].astype(jnp.float32), gains[3:4, :]).astype(jnp.bfloat16)
        text_queries = normed(tq[...].astype(jnp.float32), gains[2:3, :])
        pltpu.make_async_copy(q_in.at[pl.ds(0, PLANE - 1)], q_in.at[pl.ds(0, PLANE - 1)], q_recv).wait()
        q = jnp.concatenate([q_in[...], text_queries.reshape(PLANE, ROWS, HD)], axis=1)
        q = q.reshape(PLANE * 2 * ROWS, HD).astype(jnp.bfloat16)
        s = scores_of(q, keys)
        valid = lax.broadcasted_iota(jnp.int32, s.shape, 1) < length_ref[0]
        s = jnp.where(valid, s, NEG)
        text_max = jnp.max(s, axis=-1, keepdims=True)
        e = jnp.exp2((s - text_max) * scale)
        text_sum = jnp.sum(e, axis=-1, keepdims=True)
        text_part = jnp.dot(e.astype(jnp.bfloat16), tv[...], preferred_element_type=jnp.float32)

        pltpu.make_async_copy(kv_in.at[pl.ds(0, SEQ - 1)], kv_in.at[pl.ds(0, SEQ - 1)], kv_recv).wait()
        kv = kv_in[...].astype(jnp.float32)
        k = kv[:, :ROWS, :].reshape(SEQ * ROWS, HD).astype(jnp.bfloat16)
        v = kv[:, ROWS:, :].reshape(SEQ * ROWS, HD).astype(jnp.bfloat16)
        s = scores_of(q, k)
        top = jnp.maximum(jnp.max(s, axis=-1, keepdims=True), text_max)
        e = jnp.exp2((s - top) * scale)
        keep = jnp.exp2((text_max - top) * scale)
        total = jnp.sum(e, axis=-1, keepdims=True) + text_sum * keep
        o = jnp.dot(e.astype(jnp.bfloat16), v, preferred_element_type=jnp.float32) + text_part * keep
        o = (o / total).astype(jnp.bfloat16)
        o_out[...] = o.reshape(PLANE, 2 * ROWS, HD)
        for i in range(1, PLANE):
            other = (spot + i) % PLANE
            pltpu.make_async_remote_copy(
                src_ref=o_out.at[other], dst_ref=o_in.at[head], send_sem=o_send, recv_sem=o_recv,
                device_id={"seq": x * 16 + other}, device_id_type=MESH).start()
        o_in[head] = o_out[spot]
        pltpu.make_async_copy(o_in.at[pl.ds(0, HEADS - 1)], o_in.at[pl.ds(0, HEADS - 1)], o_recv).wait()

    @pl.when(jnp.logical_not(owner))
    def _():
        for load in loads[4:]:
            load.wait()
        pltpu.make_async_copy(o_in, o_in, o_recv).wait()

    for h in range(HEADS):
        o = o_in[h].astype(jnp.float32)
        cols = slice(h * HD, (h + 1) * HD)
        image_out[:, cols] = o[:ROWS].astype(jnp.bfloat16)
        text_out[:, cols] = o[ROWS:].astype(jnp.bfloat16)

    def drain(ref, count, sem):
        pltpu.make_async_copy(ref.at[pl.ds(0, count)], ref.at[pl.ds(0, count)], sem).wait()

    drain(kv_in, 47, kv_send)
    drain(q_in, 11, q_send)

    @pl.when(owner)
    def _():
        drain(o_out, PLANE - 1, o_send)

    @pl.when(jnp.logical_not(owner))
    def _():
        drain(kv_in, 1, kv_send)
        drain(q_in, 1, q_send)


def local(image_query, image_key, image_value, text_query, text_key, text_value, image_query_gain,
          image_key_gain, text_query_gain, text_key_gain, image_order, text_length):
    gains = jnp.stack([image_query_gain, image_key_gain, text_query_gain, text_key_gain])
    hbm = pl.BlockSpec(memory_space=pl.ANY)
    smem = pl.BlockSpec(memory_space=pltpu.SMEM)
    vmem = pl.BlockSpec(memory_space=pltpu.VMEM)
    bf16, f32 = jnp.bfloat16, jnp.float32
    width = image_query.shape[1]
    text_rows = text_key.shape[0]
    out = jax.ShapeDtypeStruct((ROWS, width), bf16)
    dma = pltpu.SemaphoreType.DMA
    return pl.pallas_call(
        kernel,
        out_shape=(out, out),
        in_specs=[smem, smem] + [hbm] * 7,
        out_specs=(vmem, vmem),
        scratch_shapes=[
            pltpu.VMEM((ROWS, width), bf16),
            pltpu.VMEM((ROWS, width), bf16),
            pltpu.VMEM((ROWS, width), bf16),
            pltpu.VMEM((PLANE * ROWS, HD), bf16),
            pltpu.VMEM((text_rows, HD), bf16),
            pltpu.VMEM((text_rows, HD), bf16),
            pltpu.VMEM((4, HD), f32),
            pltpu.VMEM((HEADS, 2 * ROWS, HD), bf16),
            pltpu.VMEM((HEADS, ROWS, HD), f32),
            pltpu.VMEM((SEQ, 2 * ROWS, HD), bf16),
            pltpu.VMEM((PLANE, ROWS, HD), f32),
            pltpu.VMEM((PLANE, 2 * ROWS, HD), bf16),
            pltpu.VMEM((HEADS, 2 * ROWS, HD), bf16),
            dma((7,)), dma, dma, dma, dma, dma, dma,
        ],
        compiler_params=pltpu.CompilerParams(collective_id=0, has_side_effects=True),
        name="joint",
    )(image_order, text_length, image_query, image_key, image_value, text_query, text_key, text_value, gains)


def solution(mesh):
    placed = (
        P(("req", "seq"), None),
        P(("req", "seq"), None),
        P(("req", "seq"), None),
        P("req", None),
        P("req", None),
        P("req", None),
        P(),
        P(),
        P(),
        P(),
        P(("req", "seq")),
        P("req"),
    )
    return jax.shard_map(
        local,
        mesh=mesh,
        in_specs=placed,
        out_specs=(P(("req", "seq"), None), P(("req", "seq"), None)),
        check_vma=False,
    )
```

```python
import jax
import jax.numpy as jnp
from jax import lax
from jax.experimental import pallas as pl
from jax.experimental.pallas import tpu as pltpu
from jax.sharding import PartitionSpec as P

GRID_W = 64
EPS = 1e-06
NEG = -1e30
MESH = pl.DeviceIdType.MESH
HEADS = 12
HD = 128
ROWS = 8
PLANE = 16
SEQ = 64
LOG2E = 1.4426950408889634


def at(x, z, y):
    return x * 16 + z * 4 + y


OWNERS = [at(0, 0, 0), at(0, 3, 0), at(1, 0, 0), at(1, 3, 0), at(0, 0, 1), at(0, 3, 1),
          at(3, 0, 0), at(3, 3, 0), at(0, 0, 3), at(0, 3, 3), at(2, 0, 0), at(0, 0, 2)]


def normed(x, gain):
    mean_square = jnp.mean(x * x, axis=-1, keepdims=True)
    return x * lax.rsqrt(mean_square + EPS) * gain


def lanes():
    lane = lax.broadcasted_iota(jnp.int32, (ROWS, HD), 1)
    pair = lane >> 1
    first = pair < 8
    second = pair < 36
    within = jnp.where(first, pair, jnp.where(second, pair - 8, pair - 36)).astype(jnp.float32)
    width = jnp.where(first, 16.0, 56.0).astype(jnp.float32)
    frequency = jnp.exp(within / width * jnp.float32(-2.0 * 9.210340371976184))
    return frequency, first, second, (lane & 1) == 0


def rotary(order_ref, frequency, first, second, even):
    row = lax.broadcasted_iota(jnp.int32, (ROWS, HD), 0)
    position = jnp.zeros((ROWS, HD), jnp.int32)
    for r in range(ROWS):
        position = jnp.where(row == r, order_ref[r], position)
    half = 4 * GRID_W
    inside = position & (half - 1)
    place = jnp.where(first, position >> 8, jnp.where(second, inside >> 6, inside & (GRID_W - 1)))
    angle = place.astype(jnp.float32) * frequency
    sine = jnp.sin(angle)
    return jnp.cos(angle), jnp.where(even, -sine, sine)


def turn(x, cosine, sine, even):
    other = jnp.where(even, pltpu.roll(x, HD - 1, 1), pltpu.roll(x, 1, 1))
    return x * cosine + other * sine


def scores_of(q, k):
    return lax.dot_general(q, k, (((1,), (1,)), ((), ())), preferred_element_type=jnp.float32)


def kernel(order_hbm, length_ref, iq_hbm, ik_hbm, iv_hbm, tq_hbm, tk_hbm, tv_hbm,
           iq_gain_hbm, ik_gain_hbm, tq_gain_hbm, tk_gain_hbm,
           o_in,
           order, iq, ik, iv, tq, tk, tv, gains, kv_out, q_out, kv_in, q_in, o_out,
           load_sem, kv_send, kv_recv, q_send, q_recv, o_send, o_recv):
    me = lax.axis_index("seq")
    x, z, y = me // 16, (me // 4) % 4, me % 4
    spot = z * 16 + x * 4 + y
    head = jnp.int32(0)
    owner = me == OWNERS[0]
    for h in range(1, HEADS):
        mine = me == OWNERS[h]
        head = jnp.where(mine, h, head)
        owner = jnp.logical_or(owner, mine)
    scale = HD ** -0.5 * LOG2E

    loads = [
        pltpu.make_async_copy(order_hbm, order, load_sem.at[0]),
        pltpu.make_async_copy(ik_hbm, ik, load_sem.at[1]),
        pltpu.make_async_copy(ik_gain_hbm, gains.at[1:2], load_sem.at[2]),
        pltpu.make_async_copy(iv_hbm, iv, load_sem.at[3]),
        pltpu.make_async_copy(iq_hbm, iq, load_sem.at[4]),
        pltpu.make_async_copy(iq_gain_hbm, gains.at[0:1], load_sem.at[5]),
    ]
    for load in loads:
        load.start()
    barrier = pltpu.get_barrier_semaphore()
    column = pl.ds(pl.multiple_of(head * HD, HD), HD)
    text_loads = [
        pltpu.make_async_copy(tk_gain_hbm, gains.at[3:4], load_sem.at[6]),
        pltpu.make_async_copy(tk_hbm.at[:, column], tk, load_sem.at[7]),
        pltpu.make_async_copy(tq_gain_hbm, gains.at[2:3], load_sem.at[8]),
        pltpu.make_async_copy(tq_hbm.at[:, column], tq, load_sem.at[9]),
        pltpu.make_async_copy(tv_hbm.at[:, column], tv, load_sem.at[10]),
    ]

    @pl.when(owner)
    def _():
        def greet(i, c):
            pl.semaphore_signal(barrier, inc=1, device_id={"seq": (me + i) % SEQ}, device_id_type=MESH)
            return c

        lax.fori_loop(1, SEQ, greet, 0)
        for load in text_loads:
            load.start()

    frequency, first, second, even = lanes()
    loads[0].wait()
    cosine, sine = rotary(order, frequency, first, second, even)
    for load in loads[1:4]:
        load.wait()

    for h in range(HEADS):
        cols = slice(h * HD, (h + 1) * HD)
        k = turn(normed(ik[:, cols].astype(jnp.float32), gains[1:2, :]), cosine, sine, even)
        v = iv[:, cols].astype(jnp.float32)
        kv_out[h] = jnp.concatenate([k, v], axis=0).astype(jnp.bfloat16)

    @pl.when(owner)
    def _():
        pl.semaphore_wait(barrier, HEADS - 1)

    @pl.when(jnp.logical_not(owner))
    def _():
        pl.semaphore_wait(barrier, HEADS)

    for h in range(HEADS):
        @pl.when(me != OWNERS[h])
        def _():
            pltpu.make_async_remote_copy(
                src_ref=kv_out.at[h], dst_ref=kv_in.at[spot], send_sem=kv_send, recv_sem=kv_recv.at[z],
                device_id={"seq": OWNERS[h]}, device_id_type=MESH).start()

    for load in loads[4:]:
        load.wait()
    for h in range(HEADS):
        cols = slice(h * HD, (h + 1) * HD)
        q = turn(normed(iq[:, cols].astype(jnp.float32), gains[0:1, :]), cosine, sine, even)
        q_out[h] = q.astype(jnp.bfloat16)
    for h in range(HEADS):
        @pl.when(me != OWNERS[h])
        def _():
            pltpu.make_async_remote_copy(
                src_ref=q_out.at[h], dst_ref=q_in.at[spot], send_sem=q_send, recv_sem=q_recv.at[z],
                device_id={"seq": OWNERS[h]}, device_id_type=MESH).start()

    def drain(ref, count, sem):
        pltpu.make_async_copy(ref.at[pl.ds(0, count)], ref.at[pl.ds(0, count)], sem).wait()

    def arrived(ref, sem, group):
        @pl.when(z == group)
        def _():
            drain(ref, PLANE - 1, sem.at[group])

        @pl.when(z != group)
        def _():
            drain(ref, PLANE, sem.at[group])

    @pl.when(owner)
    def _():
        kv_in[spot] = kv_out[head]
        q_in[spot] = q_out[head]
        for load in text_loads:
            load.wait()
        text_keys = normed(tk[...].astype(jnp.float32), gains[3:4, :]).astype(jnp.bfloat16)
        text_queries = normed(tq[...].astype(jnp.float32), gains[2:3, :])
        text_values = tv[...]

        def queries(group):
            image = q_in[pl.ds(group * PLANE, PLANE)].astype(jnp.float32)
            text = jnp.concatenate(
                [text_queries[i * 128 + group * 32:i * 128 + group * 32 + 32] for i in range(4)], axis=0)
            both = jnp.concatenate([image, text.reshape(PLANE, ROWS, HD)], axis=1)
            return both.reshape(PLANE * 2 * ROWS, HD).astype(jnp.bfloat16)

        def text_part(q):
            s = scores_of(q, text_keys)
            valid = lax.broadcasted_iota(jnp.int32, s.shape, 1) < length_ref[0]
            s = jnp.where(valid, s, NEG)
            top = jnp.max(s, axis=-1, keepdims=True)
            e = jnp.exp2((s - top) * scale)
            total = jnp.sum(e, axis=-1, keepdims=True)
            return top, total, jnp.dot(e.astype(jnp.bfloat16), text_values, preferred_element_type=jnp.float32)

        early = {}
        for group in (0, 1):
            arrived(q_in, q_recv, group)
            q = queries(group)
            early[group] = (q, text_part(q))
        for group in range(4):
            arrived(kv_in, kv_recv, group)
        kv = kv_in[...].astype(jnp.float32)
        k = kv[:, :ROWS, :].reshape(SEQ * ROWS, HD).astype(jnp.bfloat16)
        v = kv[:, ROWS:, :].reshape(SEQ * ROWS, HD).astype(jnp.bfloat16)
        for group in (0, 1, 3, 2):
            if group not in early:
                arrived(q_in, q_recv, group)
                q = queries(group)
                early[group] = (q, text_part(q))
            q, (text_max, text_sum, text_out) = early[group]
            s = scores_of(q, k)
            top = jnp.maximum(jnp.max(s, axis=-1, keepdims=True), text_max)
            e = jnp.exp2((s - top) * scale)
            keep = jnp.exp2((text_max - top) * scale)
            total = jnp.sum(e, axis=-1, keepdims=True) + text_sum * keep
            o = jnp.dot(e.astype(jnp.bfloat16), v, preferred_element_type=jnp.float32) + text_out * keep
            o = (o / total).astype(jnp.bfloat16)
            o_out[pl.ds(group * PLANE, PLANE)] = o.reshape(PLANE, 2 * ROWS, HD)
            for i in range(PLANE):
                to = at(i // 4, group, i % 4)

                def send():
                    pltpu.make_async_remote_copy(
                        src_ref=o_out.at[group * PLANE + i], dst_ref=o_in.at[head], send_sem=o_send,
                        recv_sem=o_recv, device_id={"seq": to}, device_id_type=MESH).start()

                if to in OWNERS:
                    pl.when(me != to)(send)
                else:
                    send()
        o_in[head] = o_out[spot]
        drain(o_in, HEADS - 1, o_recv)
        drain(kv_out, HEADS - 1, kv_send)
        drain(q_out, HEADS - 1, q_send)
        drain(o_out, SEQ - 1, o_send)

    @pl.when(jnp.logical_not(owner))
    def _():
        drain(o_in, HEADS, o_recv)
        drain(kv_out, HEADS, kv_send)
        drain(q_out, HEADS, q_send)


def spread(o_in, image_hbm, text_hbm, image, text, sem):
    for h in range(HEADS):
        o = o_in[h].astype(jnp.float32)
        cols = slice(h * HD, (h + 1) * HD)
        image[:, cols] = o[:ROWS].astype(jnp.bfloat16)
        text[:, cols] = o[ROWS:].astype(jnp.bfloat16)
    stores = [pltpu.make_async_copy(image, image_hbm, sem.at[0]), pltpu.make_async_copy(text, text_hbm, sem.at[1])]
    for store in stores:
        store.start()
    for store in stores:
        store.wait()


def local(image_query, image_key, image_value, text_query, text_key, text_value, image_query_gain,
          image_key_gain, text_query_gain, text_key_gain, image_order, text_length):
    hbm = pl.BlockSpec(memory_space=pl.ANY)
    smem = pl.BlockSpec(memory_space=pltpu.SMEM)
    vmem = pl.BlockSpec(memory_space=pltpu.VMEM)
    bf16, f32 = jnp.bfloat16, jnp.float32
    width = image_query.shape[1]
    text_rows = text_key.shape[0]
    dma = pltpu.SemaphoreType.DMA
    gains = [g.reshape(1, HD) for g in (image_query_gain, image_key_gain, text_query_gain, text_key_gain)]
    blocks = pl.pallas_call(
        kernel,
        out_shape=pltpu.VMEM((HEADS, 2 * ROWS, HD), bf16),
        in_specs=[hbm, smem] + [hbm] * 10,
        out_specs=vmem,
        scratch_shapes=[
            pltpu.SMEM((ROWS,), jnp.int32),
            pltpu.VMEM((ROWS, width), bf16),
            pltpu.VMEM((ROWS, width), bf16),
            pltpu.VMEM((ROWS, width), bf16),
            pltpu.VMEM((text_rows, HD), bf16),
            pltpu.VMEM((text_rows, HD), bf16),
            pltpu.VMEM((text_rows, HD), bf16),
            pltpu.VMEM((4, HD), f32),
            pltpu.VMEM((HEADS, 2 * ROWS, HD), bf16),
            pltpu.VMEM((HEADS, ROWS, HD), bf16),
            pltpu.VMEM((SEQ, 2 * ROWS, HD), bf16),
            pltpu.VMEM((SEQ, ROWS, HD), bf16),
            pltpu.VMEM((SEQ, 2 * ROWS, HD), bf16),
            dma((11,)), dma, dma((4,)), dma, dma((4,)), dma, dma,
        ],
        compiler_params=pltpu.CompilerParams(collective_id=0, has_side_effects=True),
        name="joint",
    )(image_order, text_length, image_query, image_key, image_value, text_query, text_key, text_value, *gains)
    out = jax.ShapeDtypeStruct((ROWS, width), bf16)
    return pl.pallas_call(
        spread,
        out_shape=(out, out),
        in_specs=[vmem],
        out_specs=(hbm, hbm),
        scratch_shapes=[pltpu.VMEM((ROWS, width), bf16), pltpu.VMEM((ROWS, width), bf16), dma((2,))],
        name="spread",
    )(pltpu.with_memory_space_constraint(blocks, pltpu.VMEM))


def solution(mesh):
    placed = (
        P(("req", "seq"), None),
        P(("req", "seq"), None),
        P(("req", "seq"), None),
        P("req", None),
        P("req", None),
        P("req", None),
        P(),
        P(),
        P(),
        P(),
        P(("req", "seq")),
        P("req"),
    )
    return jax.shard_map(
        local,
        mesh=mesh,
        in_specs=placed,
        out_specs=(P(("req", "seq"), None), P(("req", "seq"), None)),
        check_vma=False,
    )
```

```python
import jax
import jax.numpy as jnp
from jax import lax
from jax.experimental import pallas as pl
from jax.experimental.pallas import tpu as pltpu
from jax.sharding import PartitionSpec as P

GRID_W = 64
EPS = 1e-06
NEG = -1e30
MESH = pl.DeviceIdType.MESH
HEADS = 12
HD = 128
ROWS = 8
PLANE = 16
SEQ = 64
LOG2E = 1.4426950408889634


def at(x, z, y):
    return x * 16 + z * 4 + y


OWNERS = (
    [at(0, 0, 0), at(1, 0, 0), at(0, 0, 1), at(0, 1, 0), at(1, 0, 1), at(1, 1, 0),
     at(0, 1, 1), at(2, 0, 0), at(0, 0, 2), at(0, 2, 0), at(1, 1, 1), at(3, 0, 0)],
    [at(0, 0, 3), at(1, 0, 2), at(2, 0, 1), at(3, 0, 1), at(1, 0, 3), at(2, 0, 2),
     at(2, 1, 0), at(0, 1, 2), at(3, 1, 0), at(0, 1, 3), at(1, 1, 2), at(2, 1, 1)],
)
OWNING = set(OWNERS[0] + OWNERS[1])


def ring(a):
    return min(a, 4 - a)


FAR_FIRST = sorted(range(SEQ), key=lambda t: -(ring(t // 16) + 1.5 * ring(t // 4 % 4) + ring(t % 4)))


def normed(x, gain):
    mean_square = jnp.mean(x * x, axis=-1, keepdims=True)
    return x * lax.rsqrt(mean_square + EPS) * gain


def lanes():
    lane = lax.broadcasted_iota(jnp.int32, (ROWS, HD), 1)
    pair = lane >> 1
    first = pair < 8
    second = pair < 36
    within = jnp.where(first, pair, jnp.where(second, pair - 8, pair - 36)).astype(jnp.float32)
    width = jnp.where(first, 16.0, 56.0).astype(jnp.float32)
    frequency = jnp.exp(within / width * jnp.float32(-2.0 * 9.210340371976184))
    return frequency, first, second, (lane & 1) == 0


def rotary(order_ref, frequency, first, second, even):
    row = lax.broadcasted_iota(jnp.int32, (ROWS, HD), 0)
    position = jnp.zeros((ROWS, HD), jnp.int32)
    for r in range(ROWS):
        position = jnp.where(row == r, order_ref[r], position)
    half = 4 * GRID_W
    inside = position & (half - 1)
    place = jnp.where(first, position >> 8, jnp.where(second, inside >> 6, inside & (GRID_W - 1)))
    angle = place.astype(jnp.float32) * frequency
    sine = jnp.sin(angle)
    return jnp.cos(angle), jnp.where(even, -sine, sine)


def turn(x, cosine, sine, even):
    other = jnp.where(even, pltpu.roll(x, HD - 1, 1), pltpu.roll(x, 1, 1))
    return x * cosine + other * sine


def scores_of(q, k):
    return lax.dot_general(q, k, (((1,), (1,)), ((), ())), preferred_element_type=jnp.float32)


def kernel(order_hbm, length_ref, iq_hbm, ik_hbm, iv_hbm, tq_hbm, tk_hbm, tv_hbm,
           iq_gain_hbm, ik_gain_hbm, tq_gain_hbm, tk_gain_hbm,
           o_in,
           order, iq, ik, iv, tq, tk, tv, gains, kv_out, q_out, kv_in, q_in, o_out,
           load_sem, kv_send, kv_recv, q_send, q_recv, o_send, o_recv):
    me = lax.axis_index("seq")
    x, z, y = me // 16, (me // 4) % 4, me % 4
    spot = z * 16 + x * 4 + y
    other_request = lax.axis_index("req") == 1
    owners = [jnp.where(other_request, b, a) for a, b in zip(*OWNERS)]
    head = jnp.int32(0)
    owner = me == owners[0]
    for h in range(1, HEADS):
        mine = me == owners[h]
        head = jnp.where(mine, h, head)
        owner = jnp.logical_or(owner, mine)
    scale = HD ** -0.5 * LOG2E

    loads = [
        pltpu.make_async_copy(order_hbm, order, load_sem.at[0]),
        pltpu.make_async_copy(ik_hbm, ik, load_sem.at[1]),
        pltpu.make_async_copy(ik_gain_hbm, gains.at[1:2], load_sem.at[2]),
        pltpu.make_async_copy(iv_hbm, iv, load_sem.at[3]),
        pltpu.make_async_copy(iq_hbm, iq, load_sem.at[4]),
        pltpu.make_async_copy(iq_gain_hbm, gains.at[0:1], load_sem.at[5]),
    ]
    for load in loads:
        load.start()
    barrier = pltpu.get_barrier_semaphore()
    column = pl.ds(pl.multiple_of(head * HD, HD), HD)
    text_loads = [
        pltpu.make_async_copy(tk_gain_hbm, gains.at[3:4], load_sem.at[6]),
        pltpu.make_async_copy(tk_hbm.at[:, column], tk, load_sem.at[7]),
        pltpu.make_async_copy(tq_gain_hbm, gains.at[2:3], load_sem.at[8]),
        pltpu.make_async_copy(tq_hbm.at[:, column], tq, load_sem.at[9]),
        pltpu.make_async_copy(tv_hbm.at[:, column], tv, load_sem.at[10]),
    ]

    @pl.when(owner)
    def _():
        with jax.named_scope("b_greet"):
            for t in FAR_FIRST:
                def greet():
                    pl.semaphore_signal(barrier, inc=1, device_id={"seq": t}, device_id_type=MESH)

                if t in OWNING:
                    pl.when(me != t)(greet)
                else:
                    greet()
        for load in text_loads:
            load.start()

    frequency, first, second, even = lanes()
    with jax.named_scope("c_loads"):
        for load in loads[:4]:
            load.wait()
    with jax.named_scope("e_kv"):
        cosine, sine = rotary(order, frequency, first, second, even)
        for h in range(HEADS):
            cols = slice(h * HD, (h + 1) * HD)
            k = turn(normed(ik[:, cols].astype(jnp.float32), gains[1:2, :]), cosine, sine, even)
            v = iv[:, cols].astype(jnp.float32)
            kv_out[h] = jnp.concatenate([k, v], axis=0).astype(jnp.bfloat16)

    with jax.named_scope("f_barrier"):
        @pl.when(owner)
        def _():
            pl.semaphore_wait(barrier, HEADS - 1)

        @pl.when(jnp.logical_not(owner))
        def _():
            pl.semaphore_wait(barrier, HEADS)

    for h in range(HEADS):
        @pl.when(me != owners[h])
        def _():
            pltpu.make_async_remote_copy(
                src_ref=kv_out.at[h], dst_ref=kv_in.at[spot], send_sem=kv_send, recv_sem=kv_recv.at[z],
                device_id={"seq": owners[h]}, device_id_type=MESH).start()

    for load in loads[4:]:
        load.wait()
    for h in range(HEADS):
        cols = slice(h * HD, (h + 1) * HD)
        q = turn(normed(iq[:, cols].astype(jnp.float32), gains[0:1, :]), cosine, sine, even)
        q_out[h] = q.astype(jnp.bfloat16)
    for h in range(HEADS):
        @pl.when(me != owners[h])
        def _():
            pltpu.make_async_remote_copy(
                src_ref=q_out.at[h], dst_ref=q_in.at[spot], send_sem=q_send, recv_sem=q_recv.at[z],
                device_id={"seq": owners[h]}, device_id_type=MESH).start()

    def drain(ref, count, sem):
        pltpu.make_async_copy(ref.at[pl.ds(0, count)], ref.at[pl.ds(0, count)], sem).wait()

    def arrived(ref, sem, group):
        @pl.when(z == group)
        def _():
            drain(ref, PLANE - 1, sem.at[group])

        @pl.when(z != group)
        def _():
            drain(ref, PLANE, sem.at[group])

    @pl.when(owner)
    def _():
        kv_in[spot] = kv_out[head]
        q_in[spot] = q_out[head]
        for load in text_loads:
            load.wait()
        text_keys = normed(tk[...].astype(jnp.float32), gains[3:4, :]).astype(jnp.bfloat16)
        text_queries = normed(tq[...].astype(jnp.float32), gains[2:3, :])
        text_values = tv[...]

        def queries(group):
            image = q_in[pl.ds(group * PLANE, PLANE)].astype(jnp.float32)
            text = jnp.concatenate(
                [text_queries[i * 128 + group * 32:i * 128 + group * 32 + 32] for i in range(4)], axis=0)
            both = jnp.concatenate([image, text.reshape(PLANE, ROWS, HD)], axis=1)
            return both.reshape(PLANE * 2 * ROWS, HD).astype(jnp.bfloat16)

        def text_part(q):
            s = scores_of(q, text_keys)
            valid = lax.broadcasted_iota(jnp.int32, s.shape, 1) < length_ref[0]
            s = jnp.where(valid, s, NEG)
            top = jnp.max(s, axis=-1, keepdims=True)
            e = jnp.exp2((s - top) * scale)
            total = jnp.sum(e, axis=-1, keepdims=True)
            return top, total, jnp.dot(e.astype(jnp.bfloat16), text_values, preferred_element_type=jnp.float32)

        early = {}
        for group in (0, 1):
            with jax.named_scope("k%d_q" % group):
                arrived(q_in, q_recv, group)
            with jax.named_scope("k%d_text" % group):
                q = queries(group)
                early[group] = (q, text_part(q))
        for group in (0, 1, 3, 2):
            with jax.named_scope("l%d_kv" % group):
                arrived(kv_in, kv_recv, group)
        kv = kv_in[...].astype(jnp.float32)
        k = kv[:, :ROWS, :].reshape(SEQ * ROWS, HD).astype(jnp.bfloat16)
        v = kv[:, ROWS:, :].reshape(SEQ * ROWS, HD).astype(jnp.bfloat16)
        for group in (0, 1, 3, 2):
            if group not in early:
                with jax.named_scope("n%d_q" % group):
                    arrived(q_in, q_recv, group)
                with jax.named_scope("n%d_text" % group):
                    q = queries(group)
                    early[group] = (q, text_part(q))
            with jax.named_scope("n%d_image" % group):
                q, (text_max, text_sum, text_out) = early[group]
                s = scores_of(q, k)
                top = jnp.maximum(jnp.max(s, axis=-1, keepdims=True), text_max)
                e = jnp.exp2((s - top) * scale)
                keep = jnp.exp2((text_max - top) * scale)
                total = jnp.sum(e, axis=-1, keepdims=True) + text_sum * keep
                o = jnp.dot(e.astype(jnp.bfloat16), v, preferred_element_type=jnp.float32) + text_out * keep
                o = (o / total).astype(jnp.bfloat16)
                o_out[pl.ds(group * PLANE, PLANE)] = o.reshape(PLANE, 2 * ROWS, HD)
            with jax.named_scope("n%d_send" % group):
                for i in range(PLANE):
                    to = at(i // 4, group, i % 4)

                    def send():
                        pltpu.make_async_remote_copy(
                            src_ref=o_out.at[group * PLANE + i], dst_ref=o_in.at[head], send_sem=o_send,
                            recv_sem=o_recv, device_id={"seq": to}, device_id_type=MESH).start()

                    if to in OWNING:
                        pl.when(me != to)(send)
                    else:
                        send()
        o_in[head] = o_out[spot]
        with jax.named_scope("o_wait"):
            drain(o_in, HEADS - 1, o_recv)
        drain(kv_out, HEADS - 1, kv_send)
        drain(q_out, HEADS - 1, q_send)
        drain(o_out, SEQ - 1, o_send)

    @pl.when(jnp.logical_not(owner))
    def _():
        with jax.named_scope("p_wait"):
            drain(o_in, HEADS, o_recv)
        drain(kv_out, HEADS, kv_send)
        drain(q_out, HEADS, q_send)


def spread(o_in, image_hbm, text_hbm, image, text, sem):
    for h in range(HEADS):
        o = o_in[h].astype(jnp.float32)
        cols = slice(h * HD, (h + 1) * HD)
        image[:, cols] = o[:ROWS].astype(jnp.bfloat16)
        text[:, cols] = o[ROWS:].astype(jnp.bfloat16)
    stores = [pltpu.make_async_copy(image, image_hbm, sem.at[0]), pltpu.make_async_copy(text, text_hbm, sem.at[1])]
    for store in stores:
        store.start()
    for store in stores:
        store.wait()


def local(image_query, image_key, image_value, text_query, text_key, text_value, image_query_gain,
          image_key_gain, text_query_gain, text_key_gain, image_order, text_length):
    hbm = pl.BlockSpec(memory_space=pl.ANY)
    smem = pl.BlockSpec(memory_space=pltpu.SMEM)
    vmem = pl.BlockSpec(memory_space=pltpu.VMEM)
    bf16, f32 = jnp.bfloat16, jnp.float32
    width = image_query.shape[1]
    text_rows = text_key.shape[0]
    dma = pltpu.SemaphoreType.DMA
    gains = [g.reshape(1, HD) for g in (image_query_gain, image_key_gain, text_query_gain, text_key_gain)]
    blocks = pl.pallas_call(
        kernel,
        out_shape=pltpu.VMEM((HEADS, 2 * ROWS, HD), bf16),
        in_specs=[hbm, smem] + [hbm] * 10,
        out_specs=vmem,
        scratch_shapes=[
            pltpu.SMEM((ROWS,), jnp.int32),
            pltpu.VMEM((ROWS, width), bf16),
            pltpu.VMEM((ROWS, width), bf16),
            pltpu.VMEM((ROWS, width), bf16),
            pltpu.VMEM((text_rows, HD), bf16),
            pltpu.VMEM((text_rows, HD), bf16),
            pltpu.VMEM((text_rows, HD), bf16),
            pltpu.VMEM((4, HD), f32),
            pltpu.VMEM((HEADS, 2 * ROWS, HD), bf16),
            pltpu.VMEM((HEADS, ROWS, HD), bf16),
            pltpu.VMEM((SEQ, 2 * ROWS, HD), bf16),
            pltpu.VMEM((SEQ, ROWS, HD), bf16),
            pltpu.VMEM((SEQ, 2 * ROWS, HD), bf16),
            dma((11,)), dma, dma((4,)), dma, dma((4,)), dma, dma,
        ],
        compiler_params=pltpu.CompilerParams(collective_id=0, has_side_effects=True),
        name="joint",
    )(image_order, text_length, image_query, image_key, image_value, text_query, text_key, text_value, *gains)
    out = jax.ShapeDtypeStruct((ROWS, width), bf16)
    return pl.pallas_call(
        spread,
        out_shape=(out, out),
        in_specs=[vmem],
        out_specs=(hbm, hbm),
        scratch_shapes=[pltpu.VMEM((ROWS, width), bf16), pltpu.VMEM((ROWS, width), bf16), dma((2,))],
        name="spread",
    )(pltpu.with_memory_space_constraint(blocks, pltpu.VMEM))


def solution(mesh):
    placed = (
        P(("req", "seq"), None),
        P(("req", "seq"), None),
        P(("req", "seq"), None),
        P("req", None),
        P("req", None),
        P("req", None),
        P(),
        P(),
        P(),
        P(),
        P(("req", "seq")),
        P("req"),
    )
    return jax.shard_map(
        local,
        mesh=mesh,
        in_specs=placed,
        out_specs=(P(("req", "seq"), None), P(("req", "seq"), None)),
        check_vma=False,
    )
```

```python
import jax
import jax.numpy as jnp
from jax import lax
from jax.experimental import pallas as pl
from jax.experimental.pallas import tpu as pltpu
from jax.sharding import PartitionSpec as P

GRID_W = 64
EPS = 1e-06
NEG = -1e30
MESH = pl.DeviceIdType.MESH
HEADS = 12
HD = 128
ROWS = 8
PLANE = 16
SEQ = 64
LOG2E = 1.4426950408889634


def at(x, z, y):
    return x * 16 + z * 4 + y


OWNERS = (
    [at(0, 0, 0), at(1, 0, 0), at(0, 0, 1), at(0, 1, 0), at(3, 0, 0), at(1, 0, 1),
     at(0, 0, 2), at(2, 0, 0), at(1, 1, 0), at(2, 0, 1), at(0, 1, 1), at(0, 0, 3)],
    [at(3, 0, 1), at(1, 0, 2), at(1, 0, 3), at(2, 1, 0), at(2, 0, 2), at(3, 1, 0),
     at(0, 1, 2), at(1, 1, 1), at(0, 1, 3), at(2, 1, 1), at(1, 1, 2), at(3, 1, 1)],
)
OWNING = set(OWNERS[0] + OWNERS[1])


def ring(a):
    return min(a, 4 - a)


FAR_FIRST = sorted([(t // 16, t // 4 % 4, t % 4) for t in range(1, SEQ)], key=lambda d: -sum(map(ring, d)))


def normed(x, gain):
    mean_square = jnp.mean(x * x, axis=-1, keepdims=True)
    return x * lax.rsqrt(mean_square + EPS) * gain


def lanes():
    lane = lax.broadcasted_iota(jnp.int32, (ROWS, HD), 1)
    pair = lane >> 1
    first = pair < 8
    second = pair < 36
    within = jnp.where(first, pair, jnp.where(second, pair - 8, pair - 36)).astype(jnp.float32)
    width = jnp.where(first, 16.0, 56.0).astype(jnp.float32)
    frequency = jnp.exp(within / width * jnp.float32(-2.0 * 9.210340371976184))
    return frequency, first, second, (lane & 1) == 0


def rotary(order_ref, frequency, first, second, even):
    row = lax.broadcasted_iota(jnp.int32, (ROWS, HD), 0)
    position = jnp.zeros((ROWS, HD), jnp.int32)
    for r in range(ROWS):
        position = jnp.where(row == r, order_ref[r], position)
    half = 4 * GRID_W
    inside = position & (half - 1)
    place = jnp.where(first, position >> 8, jnp.where(second, inside >> 6, inside & (GRID_W - 1)))
    angle = place.astype(jnp.float32) * frequency
    sine = jnp.sin(angle)
    return jnp.cos(angle), jnp.where(even, -sine, sine)


def turn(x, cosine, sine, even):
    other = jnp.where(even, pltpu.roll(x, HD - 1, 1), pltpu.roll(x, 1, 1))
    return x * cosine + other * sine


def scores_of(q, k):
    return lax.dot_general(q, k, (((1,), (1,)), ((), ())), preferred_element_type=jnp.float32)


def kernel(order_hbm, length_hbm, iq_hbm, ik_hbm, iv_hbm, tq_hbm, tk_hbm, tv_hbm,
           iq_gain_hbm, ik_gain_hbm, tq_gain_hbm, tk_gain_hbm,
           o_in,
           order, length, iq, ik, iv, tq, tk, tv, gains, kv_out, q_out, kv_in, q_in, o_out,
           load_sem, kv_send, kv_recv, q_send, q_recv, o_send, o_recv):
    me = lax.axis_index("seq")
    x, z, y = me // 16, (me // 4) % 4, me % 4
    spot = z * 16 + x * 4 + y
    other_request = lax.axis_index("req") == 1
    owners = [jnp.where(other_request, b, a) for a, b in zip(*OWNERS)]
    head = jnp.int32(0)
    owner = me == owners[0]
    for h in range(1, HEADS):
        mine = me == owners[h]
        head = jnp.where(mine, h, head)
        owner = jnp.logical_or(owner, mine)
    scale = HD ** -0.5 * LOG2E

    loads = [
        pltpu.make_async_copy(order_hbm, order, load_sem.at[0]),
        pltpu.make_async_copy(ik_hbm, ik, load_sem.at[1]),
        pltpu.make_async_copy(ik_gain_hbm, gains.at[1:2], load_sem.at[2]),
        pltpu.make_async_copy(iv_hbm, iv, load_sem.at[3]),
        pltpu.make_async_copy(iq_hbm, iq, load_sem.at[4]),
        pltpu.make_async_copy(iq_gain_hbm, gains.at[0:1], load_sem.at[5]),
    ]
    for load in loads:
        load.start()
    barrier = pltpu.get_barrier_semaphore()
    column = pl.ds(pl.multiple_of(head * HD, HD), HD)
    text_loads = [
        pltpu.make_async_copy(length_hbm, length, load_sem.at[11]),
        pltpu.make_async_copy(tk_gain_hbm, gains.at[3:4], load_sem.at[6]),
        pltpu.make_async_copy(tk_hbm.at[:, column], tk, load_sem.at[7]),
        pltpu.make_async_copy(tq_gain_hbm, gains.at[2:3], load_sem.at[8]),
        pltpu.make_async_copy(tq_hbm.at[:, column], tq, load_sem.at[9]),
        pltpu.make_async_copy(tv_hbm.at[:, column], tv, load_sem.at[10]),
    ]

    @pl.when(owner)
    def _():
        with jax.named_scope("b_greet"):
            xs = [(x + d) % 4 * 16 for d in range(4)]
            zs = [(z + d) % 4 * 4 for d in range(4)]
            ys = [(y + d) % 4 for d in range(4)]
            for dx, dz, dy in FAR_FIRST:
                pl.semaphore_signal(
                    barrier, inc=1, device_id={"seq": xs[dx] + zs[dz] + ys[dy]}, device_id_type=MESH)
        for load in text_loads:
            load.start()

    frequency, first, second, even = lanes()
    with jax.named_scope("c_loads"):
        for load in loads[:4]:
            load.wait()
    with jax.named_scope("e_kv"):
        cosine, sine = rotary(order, frequency, first, second, even)
        for h in range(HEADS):
            cols = slice(h * HD, (h + 1) * HD)
            k = turn(normed(ik[:, cols].astype(jnp.float32), gains[1:2, :]), cosine, sine, even)
            v = iv[:, cols].astype(jnp.float32)
            kv_out[h] = jnp.concatenate([k, v], axis=0).astype(jnp.bfloat16)

    with jax.named_scope("f_barrier"):
        @pl.when(owner)
        def _():
            pl.semaphore_wait(barrier, HEADS - 1)

        @pl.when(jnp.logical_not(owner))
        def _():
            pl.semaphore_wait(barrier, HEADS)

    for h in range(HEADS):
        @pl.when(me != owners[h])
        def _():
            pltpu.make_async_remote_copy(
                src_ref=kv_out.at[h], dst_ref=kv_in.at[spot], send_sem=kv_send, recv_sem=kv_recv.at[z],
                device_id={"seq": owners[h]}, device_id_type=MESH).start()

    for load in loads[4:]:
        load.wait()
    for h in range(HEADS):
        cols = slice(h * HD, (h + 1) * HD)
        q = turn(normed(iq[:, cols].astype(jnp.float32), gains[0:1, :]), cosine, sine, even)
        q_out[h] = q.astype(jnp.bfloat16)
    for h in range(HEADS):
        @pl.when(me != owners[h])
        def _():
            pltpu.make_async_remote_copy(
                src_ref=q_out.at[h], dst_ref=q_in.at[spot], send_sem=q_send, recv_sem=q_recv.at[z],
                device_id={"seq": owners[h]}, device_id_type=MESH).start()

    def drain(ref, count, sem):
        pltpu.make_async_copy(ref.at[pl.ds(0, count)], ref.at[pl.ds(0, count)], sem).wait()

    def arrived(ref, sem, group):
        @pl.when(z == group)
        def _():
            drain(ref, PLANE - 1, sem.at[group])

        @pl.when(z != group)
        def _():
            drain(ref, PLANE, sem.at[group])

    @pl.when(owner)
    def _():
        kv_in[spot] = kv_out[head]
        q_in[spot] = q_out[head]
        for load in text_loads:
            load.wait()
        with jax.named_scope("j_text"):
            text_keys = normed(tk[...].astype(jnp.float32), gains[3:4, :]).astype(jnp.bfloat16)
            text_values = tv[...]
            valid = lax.broadcasted_iota(jnp.int32, (1, text_keys.shape[0]), 1) < length[0]

            def text_part(q):
                s = jnp.where(valid, scores_of(q, text_keys), NEG)
                top = jnp.max(s, axis=-1, keepdims=True)
                e = jnp.exp2((s - top) * scale)
                total = jnp.sum(e, axis=-1, keepdims=True)
                return top, total, jnp.dot(e.astype(jnp.bfloat16), text_values, preferred_element_type=jnp.float32)

            half = PLANE * ROWS
            text_queries, text_state = {}, {}
            for group in range(4):
                rows = jnp.concatenate(
                    [tq[pl.ds(i * half + group * 32, 32), :] for i in range(4)], axis=0).astype(jnp.float32)
                text_queries[group] = normed(rows, gains[2:3, :]).astype(jnp.bfloat16)

        def both_parts(first, second):
            parts = text_part(jnp.concatenate([first, second], axis=0))
            return tuple(part[:half] for part in parts), tuple(part[half:] for part in parts)

        def image_queries(group):
            return q_in[pl.ds(group * PLANE, PLANE)].astype(jnp.float32).reshape(half, HD).astype(jnp.bfloat16)

        image_q, image_state = {}, {}
        with jax.named_scope("j_part"):
            for a, b in ((0, 1), (2, 3)):
                text_state[a], text_state[b] = both_parts(text_queries[a], text_queries[b])

        def image_part(a, b):
            for group in (a, b):
                image_q[group] = image_queries(group)
            image_state[a], image_state[b] = both_parts(image_q[a], image_q[b])

        with jax.named_scope("k_q"):
            arrived(q_in, q_recv, 0)
            arrived(q_in, q_recv, 1)
        with jax.named_scope("k_text"):
            image_part(0, 1)
        with jax.named_scope("l_kv"):
            for group in (0, 1, 3, 2):
                arrived(kv_in, kv_recv, group)
        kv = kv_in[...].astype(jnp.float32)
        k = kv[:, :ROWS, :].reshape(SEQ * ROWS, HD).astype(jnp.bfloat16)
        v = kv[:, ROWS:, :].reshape(SEQ * ROWS, HD).astype(jnp.bfloat16)
        for group in (0, 1, 2, 3):
            if group == 2:
                with jax.named_scope("l_q"):
                    arrived(q_in, q_recv, 2)
                    arrived(q_in, q_recv, 3)
                with jax.named_scope("m_text"):
                    image_part(2, 3)
            with jax.named_scope("n%d_image" % group):
                q = jnp.concatenate([image_q[group], text_queries[group]], axis=0)
                text_max, text_sum, text_out = (
                    jnp.concatenate(part, axis=0) for part in zip(image_state[group], text_state[group]))
                s = scores_of(q, k)
                top = jnp.maximum(jnp.max(s, axis=-1, keepdims=True), text_max)
                e = jnp.exp2((s - top) * scale)
                keep = jnp.exp2((text_max - top) * scale)
                total = jnp.sum(e, axis=-1, keepdims=True) + text_sum * keep
                o = jnp.dot(e.astype(jnp.bfloat16), v, preferred_element_type=jnp.float32) + text_out * keep
                o = o / total
                image, text = o[:half].reshape(PLANE, ROWS, HD), o[half:].reshape(PLANE, ROWS, HD)
                o_out[pl.ds(group * PLANE, PLANE)] = jnp.concatenate([image, text], axis=1).astype(jnp.bfloat16)
            with jax.named_scope("n%d_send" % group):
                for i in range(PLANE):
                    to = at(i // 4, group, i % 4)

                    def send():
                        pltpu.make_async_remote_copy(
                            src_ref=o_out.at[group * PLANE + i], dst_ref=o_in.at[head], send_sem=o_send,
                            recv_sem=o_recv, device_id={"seq": to}, device_id_type=MESH).start()

                    if to in OWNING:
                        pl.when(me != to)(send)
                    else:
                        send()
        o_in[head] = o_out[spot]
        with jax.named_scope("o_wait"):
            drain(o_in, HEADS - 1, o_recv)
        drain(kv_out, HEADS - 1, kv_send)
        drain(q_out, HEADS - 1, q_send)
        drain(o_out, SEQ - 1, o_send)

    @pl.when(jnp.logical_not(owner))
    def _():
        with jax.named_scope("p_wait"):
            drain(o_in, HEADS, o_recv)
        drain(kv_out, HEADS, kv_send)
        drain(q_out, HEADS, q_send)


def spread(o_in, image_hbm, text_hbm, image, text, sem):
    for h in range(HEADS):
        o = o_in[h].astype(jnp.float32)
        cols = slice(h * HD, (h + 1) * HD)
        image[:, cols] = o[:ROWS].astype(jnp.bfloat16)
        text[:, cols] = o[ROWS:].astype(jnp.bfloat16)
    stores = [pltpu.make_async_copy(image, image_hbm, sem.at[0]), pltpu.make_async_copy(text, text_hbm, sem.at[1])]
    for store in stores:
        store.start()
    for store in stores:
        store.wait()


def local(image_query, image_key, image_value, text_query, text_key, text_value, image_query_gain,
          image_key_gain, text_query_gain, text_key_gain, image_order, text_length):
    hbm = pl.BlockSpec(memory_space=pl.ANY)
    vmem = pl.BlockSpec(memory_space=pltpu.VMEM)
    bf16, f32 = jnp.bfloat16, jnp.float32
    width = image_query.shape[1]
    text_rows = text_key.shape[0]
    dma = pltpu.SemaphoreType.DMA
    gains = [g.reshape(1, HD) for g in (image_query_gain, image_key_gain, text_query_gain, text_key_gain)]
    blocks = pl.pallas_call(
        kernel,
        out_shape=pltpu.VMEM((HEADS, 2 * ROWS, HD), bf16),
        in_specs=[hbm] * 12,
        out_specs=vmem,
        scratch_shapes=[
            pltpu.SMEM((ROWS,), jnp.int32),
            pltpu.SMEM((1,), jnp.int32),
            pltpu.VMEM((ROWS, width), bf16),
            pltpu.VMEM((ROWS, width), bf16),
            pltpu.VMEM((ROWS, width), bf16),
            pltpu.VMEM((text_rows, HD), bf16),
            pltpu.VMEM((text_rows, HD), bf16),
            pltpu.VMEM((text_rows, HD), bf16),
            pltpu.VMEM((4, HD), f32),
            pltpu.VMEM((HEADS, 2 * ROWS, HD), bf16),
            pltpu.VMEM((HEADS, ROWS, HD), bf16),
            pltpu.VMEM((SEQ, 2 * ROWS, HD), bf16),
            pltpu.VMEM((SEQ, ROWS, HD), bf16),
            pltpu.VMEM((SEQ, 2 * ROWS, HD), bf16),
            dma((12,)), dma, dma((4,)), dma, dma((4,)), dma, dma,
        ],
        compiler_params=pltpu.CompilerParams(collective_id=0, has_side_effects=True),
        name="joint",
    )(image_order, text_length, image_query, image_key, image_value, text_query, text_key, text_value, *gains)
    out = jax.ShapeDtypeStruct((ROWS, width), bf16)
    return pl.pallas_call(
        spread,
        out_shape=(out, out),
        in_specs=[vmem],
        out_specs=(hbm, hbm),
        scratch_shapes=[pltpu.VMEM((ROWS, width), bf16), pltpu.VMEM((ROWS, width), bf16), dma((2,))],
        name="spread",
    )(pltpu.with_memory_space_constraint(blocks, pltpu.VMEM))


def solution(mesh):
    placed = (
        P(("req", "seq"), None),
        P(("req", "seq"), None),
        P(("req", "seq"), None),
        P("req", None),
        P("req", None),
        P("req", None),
        P(),
        P(),
        P(),
        P(),
        P(("req", "seq")),
        P("req"),
    )
    return jax.shard_map(
        local,
        mesh=mesh,
        in_specs=placed,
        out_specs=(P(("req", "seq"), None), P(("req", "seq"), None)),
        check_vma=False,
    )
```

```python
import jax
import jax.numpy as jnp
from jax import lax
from jax.experimental import pallas as pl
from jax.experimental.pallas import tpu as pltpu
from jax.sharding import PartitionSpec as P

GRID_W = 64
EPS = 1e-06
NEG = -1e30
MESH = pl.DeviceIdType.MESH
HEADS = 12
HD = 128
ROWS = 8
PLANE = 16
SEQ = 64
LOG2E = 1.4426950408889634


def at(x, z, y):
    return x * 16 + z * 4 + y


OWNERS = (
    [at(0, 0, 0), at(1, 0, 0), at(0, 0, 1), at(0, 1, 0), at(3, 0, 0), at(1, 0, 1),
     at(0, 0, 2), at(2, 0, 0), at(1, 1, 0), at(2, 0, 1), at(0, 1, 1), at(0, 0, 3)],
    [at(3, 0, 1), at(1, 0, 2), at(1, 0, 3), at(2, 1, 0), at(2, 0, 2), at(3, 1, 0),
     at(0, 1, 2), at(1, 1, 1), at(0, 1, 3), at(2, 1, 1), at(1, 1, 2), at(3, 1, 1)],
)
OWNING = set(OWNERS[0] + OWNERS[1])


def ring(a):
    return min(a, 4 - a)


FAR_FIRST = sorted([(t // 16, t // 4 % 4, t % 4) for t in range(1, SEQ)], key=lambda d: -sum(map(ring, d)))


def normed(x, gain):
    mean_square = jnp.mean(x * x, axis=-1, keepdims=True)
    return x * lax.rsqrt(mean_square + EPS) * gain


def lanes():
    lane = lax.broadcasted_iota(jnp.int32, (ROWS, HD), 1)
    pair = lane >> 1
    first = pair < 8
    second = pair < 36
    within = jnp.where(first, pair, jnp.where(second, pair - 8, pair - 36)).astype(jnp.float32)
    width = jnp.where(first, 16.0, 56.0).astype(jnp.float32)
    frequency = jnp.exp(within / width * jnp.float32(-2.0 * 9.210340371976184))
    return frequency, first, second, (lane & 1) == 0


def rotary(order_ref, frequency, first, second, even):
    row = lax.broadcasted_iota(jnp.int32, (ROWS, HD), 0)
    position = jnp.zeros((ROWS, HD), jnp.int32)
    for r in range(ROWS):
        position = jnp.where(row == r, order_ref[r], position)
    half = 4 * GRID_W
    inside = position & (half - 1)
    place = jnp.where(first, position >> 8, jnp.where(second, inside >> 6, inside & (GRID_W - 1)))
    angle = place.astype(jnp.float32) * frequency
    sine = jnp.sin(angle)
    return jnp.cos(angle), jnp.where(even, -sine, sine)


def turn(x, cosine, sine, even):
    other = jnp.where(even, pltpu.roll(x, HD - 1, 1), pltpu.roll(x, 1, 1))
    return x * cosine + other * sine


def wide(column):
    return jnp.broadcast_to(column, (column.shape[0], HD))


def across(block, like):
    return jnp.concatenate([block] * (like.shape[1] // HD), axis=1)


def dot(a, b):
    return jnp.dot(a, b, preferred_element_type=jnp.float32)


def kernel(order_hbm, length_hbm, iq_hbm, ik_hbm, iv_hbm, tq_hbm, tk_hbm, tv_hbm,
           iq_gain_hbm, ik_gain_hbm, tq_gain_hbm, tk_gain_hbm,
           o_in,
           order, length, iq, ik, iv, tq, tk, tv, gains, kv_out, q_out, kv_in, q_in, keys, values, o_out,
           load_sem, kv_send, kv_recv, q_send, q_recv, o_send, o_recv):
    me = lax.axis_index("seq")
    x, z, y = me // 16, (me // 4) % 4, me % 4
    spot = z * 16 + x * 4 + y
    other_request = lax.axis_index("req") == 1
    owners = [jnp.where(other_request, b, a) for a, b in zip(*OWNERS)]
    head = jnp.int32(0)
    owner = me == owners[0]
    for h in range(1, HEADS):
        mine = me == owners[h]
        head = jnp.where(mine, h, head)
        owner = jnp.logical_or(owner, mine)
    scale = HD ** -0.5 * LOG2E

    loads = [
        pltpu.make_async_copy(order_hbm, order, load_sem.at[0]),
        pltpu.make_async_copy(ik_hbm, ik, load_sem.at[1]),
        pltpu.make_async_copy(ik_gain_hbm, gains.at[1:2], load_sem.at[2]),
        pltpu.make_async_copy(iv_hbm, iv, load_sem.at[3]),
        pltpu.make_async_copy(iq_hbm, iq, load_sem.at[4]),
        pltpu.make_async_copy(iq_gain_hbm, gains.at[0:1], load_sem.at[5]),
    ]
    for load in loads:
        load.start()
    barrier = pltpu.get_barrier_semaphore()
    column = pl.ds(pl.multiple_of(head * HD, HD), HD)
    text_loads = [
        pltpu.make_async_copy(length_hbm, length, load_sem.at[11]),
        pltpu.make_async_copy(tk_gain_hbm, gains.at[3:4], load_sem.at[6]),
        pltpu.make_async_copy(tk_hbm.at[:, column], tk, load_sem.at[7]),
        pltpu.make_async_copy(tq_gain_hbm, gains.at[2:3], load_sem.at[8]),
        pltpu.make_async_copy(tq_hbm.at[:, column], tq, load_sem.at[9]),
        pltpu.make_async_copy(tv_hbm.at[:, column], tv, load_sem.at[10]),
    ]

    @pl.when(owner)
    def _():
        with jax.named_scope("b_greet"):
            xs = [(x + d) % 4 * 16 for d in range(4)]
            zs = [(z + d) % 4 * 4 for d in range(4)]
            ys = [(y + d) % 4 for d in range(4)]
            for dx, dz, dy in FAR_FIRST:
                pl.semaphore_signal(
                    barrier, inc=1, device_id={"seq": xs[dx] + zs[dz] + ys[dy]}, device_id_type=MESH)
        for load in text_loads:
            load.start()

    frequency, first, second, even = lanes()
    with jax.named_scope("c_loads"):
        for load in loads[:4]:
            load.wait()
    with jax.named_scope("e_kv"):
        cosine, sine = rotary(order, frequency, first, second, even)
        for h in range(HEADS):
            cols = slice(h * HD, (h + 1) * HD)
            k = turn(normed(ik[:, cols].astype(jnp.float32), gains[1:2, :]), cosine, sine, even)
            v = iv[:, cols].astype(jnp.float32)
            kv_out[h] = jnp.concatenate([k, v], axis=0).astype(jnp.bfloat16)

    with jax.named_scope("f_barrier"):
        @pl.when(owner)
        def _():
            pl.semaphore_wait(barrier, HEADS - 1)

        @pl.when(jnp.logical_not(owner))
        def _():
            pl.semaphore_wait(barrier, HEADS)

    for h in range(HEADS):
        @pl.when(me != owners[h])
        def _():
            pltpu.make_async_remote_copy(
                src_ref=kv_out.at[h], dst_ref=kv_in.at[spot], send_sem=kv_send, recv_sem=kv_recv.at[z],
                device_id={"seq": owners[h]}, device_id_type=MESH).start()

    for load in loads[4:]:
        load.wait()
    for h in range(HEADS):
        cols = slice(h * HD, (h + 1) * HD)
        q = turn(normed(iq[:, cols].astype(jnp.float32), gains[0:1, :]), cosine, sine, even)
        q_out[h] = q.astype(jnp.bfloat16)
    for h in range(HEADS):
        @pl.when(me != owners[h])
        def _():
            pltpu.make_async_remote_copy(
                src_ref=q_out.at[h], dst_ref=q_in.at[spot], send_sem=q_send, recv_sem=q_recv.at[z],
                device_id={"seq": owners[h]}, device_id_type=MESH).start()

    def drain(ref, count, sem):
        pltpu.make_async_copy(ref.at[pl.ds(0, count)], ref.at[pl.ds(0, count)], sem).wait()

    def arrived(ref, sem, group):
        @pl.when(z == group)
        def _():
            drain(ref, PLANE - 1, sem.at[group])

        @pl.when(z != group)
        def _():
            drain(ref, PLANE, sem.at[group])

    @pl.when(owner)
    def _():
        kv_in[spot] = kv_out[head]
        q_in[spot] = q_out[head]
        for load in text_loads:
            load.wait()
        with jax.named_scope("j_text"):
            text_keys = normed(tk[...].astype(jnp.float32), gains[3:4, :]).T.astype(jnp.bfloat16)
            text_values = tv[...]
            valid = lax.broadcasted_iota(jnp.int32, (1, text_keys.shape[1]), 1) < length[0]

            def text_part(q):
                s = jnp.where(valid, dot(q, text_keys), NEG)
                top = wide(jnp.max(s, axis=-1, keepdims=True))
                e = jnp.exp2((s - across(top, s)) * scale)
                total = wide(jnp.sum(e, axis=-1, keepdims=True))
                return top, total, dot(e.astype(jnp.bfloat16), text_values)

            half = PLANE * ROWS
            text_queries, text_state = {}, {}
            for group in range(4):
                rows = jnp.concatenate(
                    [tq[pl.ds(i * half + group * 32, 32), :] for i in range(4)], axis=0).astype(jnp.float32)
                text_queries[group] = normed(rows, gains[2:3, :]).astype(jnp.bfloat16)

        def both_parts(first, second):
            parts = text_part(jnp.concatenate([first, second], axis=0))
            return tuple(part[:half] for part in parts), tuple(part[half:] for part in parts)

        def image_queries(group):
            return q_in[pl.ds(group * PLANE, PLANE)].astype(jnp.float32).reshape(half, HD).astype(jnp.bfloat16)

        image_q, image_state = {}, {}
        with jax.named_scope("j_part"):
            for a, b in ((0, 1), (2, 3)):
                text_state[a], text_state[b] = both_parts(text_queries[a], text_queries[b])

        def image_part(a, b):
            for group in (a, b):
                image_q[group] = image_queries(group)
            image_state[a], image_state[b] = both_parts(image_q[a], image_q[b])

        def take_keys(group):
            arrived(kv_in, kv_recv, group)
            kv = kv_in[pl.ds(group * PLANE, PLANE)].astype(jnp.float32)
            rows = pl.ds(group * half, half)
            keys[:, rows] = kv[:, :ROWS, :].reshape(half, HD).T.astype(jnp.bfloat16)
            values[rows, :] = kv[:, ROWS:, :].reshape(half, HD).astype(jnp.bfloat16)

        with jax.named_scope("k_q"):
            arrived(q_in, q_recv, 0)
            arrived(q_in, q_recv, 1)
        with jax.named_scope("k_text"):
            image_part(0, 1)
        with jax.named_scope("l_kv"):
            for group in (0, 1, 3, 2):
                take_keys(group)
        for group in (0, 1, 2, 3):
            if group == 2:
                with jax.named_scope("l_q"):
                    arrived(q_in, q_recv, 2)
                    arrived(q_in, q_recv, 3)
                with jax.named_scope("m_text"):
                    image_part(2, 3)
            with jax.named_scope("n%d_image" % group):
                q = jnp.concatenate([image_q[group], text_queries[group]], axis=0)
                text_max, text_sum, text_out = (
                    jnp.concatenate(part, axis=0) for part in zip(image_state[group], text_state[group]))
                s = dot(q, keys[...])
                top = jnp.maximum(wide(jnp.max(s, axis=-1, keepdims=True)), text_max)
                e = jnp.exp2((s - across(top, s)) * scale)
                keep = jnp.exp2((text_max - top) * scale)
                total = wide(jnp.sum(e, axis=-1, keepdims=True)) + text_sum * keep
                o = dot(e.astype(jnp.bfloat16), values[...]) + text_out * keep
                o = o / total
                image, text = o[:half].reshape(PLANE, ROWS, HD), o[half:].reshape(PLANE, ROWS, HD)
                o_out[pl.ds(group * PLANE, PLANE)] = jnp.concatenate([image, text], axis=1).astype(jnp.bfloat16)
            with jax.named_scope("n%d_send" % group):
                for i in range(PLANE):
                    to = at(i // 4, group, i % 4)

                    def send():
                        pltpu.make_async_remote_copy(
                            src_ref=o_out.at[group * PLANE + i], dst_ref=o_in.at[head], send_sem=o_send,
                            recv_sem=o_recv, device_id={"seq": to}, device_id_type=MESH).start()

                    if to in OWNING:
                        pl.when(me != to)(send)
                    else:
                        send()
        o_in[head] = o_out[spot]
        with jax.named_scope("o_wait"):
            drain(o_in, HEADS - 1, o_recv)
        drain(kv_out, HEADS - 1, kv_send)
        drain(q_out, HEADS - 1, q_send)
        drain(o_out, SEQ - 1, o_send)

    @pl.when(jnp.logical_not(owner))
    def _():
        with jax.named_scope("p_wait"):
            drain(o_in, HEADS, o_recv)
        drain(kv_out, HEADS, kv_send)
        drain(q_out, HEADS, q_send)


def spread(o_in, image_hbm, text_hbm, image, text, sem):
    for h in range(HEADS):
        o = o_in[h].astype(jnp.float32)
        cols = slice(h * HD, (h + 1) * HD)
        image[:, cols] = o[:ROWS].astype(jnp.bfloat16)
        text[:, cols] = o[ROWS:].astype(jnp.bfloat16)
    stores = [pltpu.make_async_copy(image, image_hbm, sem.at[0]), pltpu.make_async_copy(text, text_hbm, sem.at[1])]
    for store in stores:
        store.start()
    for store in stores:
        store.wait()


def local(image_query, image_key, image_value, text_query, text_key, text_value, image_query_gain,
          image_key_gain, text_query_gain, text_key_gain, image_order, text_length):
    hbm = pl.BlockSpec(memory_space=pl.ANY)
    vmem = pl.BlockSpec(memory_space=pltpu.VMEM)
    bf16, f32 = jnp.bfloat16, jnp.float32
    width = image_query.shape[1]
    text_rows = text_key.shape[0]
    dma = pltpu.SemaphoreType.DMA
    gains = [g.reshape(1, HD) for g in (image_query_gain, image_key_gain, text_query_gain, text_key_gain)]
    blocks = pl.pallas_call(
        kernel,
        out_shape=pltpu.VMEM((HEADS, 2 * ROWS, HD), bf16),
        in_specs=[hbm] * 12,
        out_specs=vmem,
        scratch_shapes=[
            pltpu.SMEM((ROWS,), jnp.int32),
            pltpu.SMEM((1,), jnp.int32),
            pltpu.VMEM((ROWS, width), bf16),
            pltpu.VMEM((ROWS, width), bf16),
            pltpu.VMEM((ROWS, width), bf16),
            pltpu.VMEM((text_rows, HD), bf16),
            pltpu.VMEM((text_rows, HD), bf16),
            pltpu.VMEM((text_rows, HD), bf16),
            pltpu.VMEM((4, HD), f32),
            pltpu.VMEM((HEADS, 2 * ROWS, HD), bf16),
            pltpu.VMEM((HEADS, ROWS, HD), bf16),
            pltpu.VMEM((SEQ, 2 * ROWS, HD), bf16),
            pltpu.VMEM((SEQ, ROWS, HD), bf16),
            pltpu.VMEM((HD, SEQ * ROWS), bf16),
            pltpu.VMEM((SEQ * ROWS, HD), bf16),
            pltpu.VMEM((SEQ, 2 * ROWS, HD), bf16),
            dma((12,)), dma, dma((4,)), dma, dma((4,)), dma, dma,
        ],
        compiler_params=pltpu.CompilerParams(collective_id=0, has_side_effects=True),
        name="joint",
    )(image_order, text_length, image_query, image_key, image_value, text_query, text_key, text_value, *gains)
    out = jax.ShapeDtypeStruct((ROWS, width), bf16)
    return pl.pallas_call(
        spread,
        out_shape=(out, out),
        in_specs=[vmem],
        out_specs=(hbm, hbm),
        scratch_shapes=[pltpu.VMEM((ROWS, width), bf16), pltpu.VMEM((ROWS, width), bf16), dma((2,))],
        name="spread",
    )(pltpu.with_memory_space_constraint(blocks, pltpu.VMEM))


def solution(mesh):
    placed = (
        P(("req", "seq"), None),
        P(("req", "seq"), None),
        P(("req", "seq"), None),
        P("req", None),
        P("req", None),
        P("req", None),
        P(),
        P(),
        P(),
        P(),
        P(("req", "seq")),
        P("req"),
    )
    return jax.shard_map(
        local,
        mesh=mesh,
        in_specs=placed,
        out_specs=(P(("req", "seq"), None), P(("req", "seq"), None)),
        check_vma=False,
    )
```

```python
import jax
import jax.numpy as jnp
from jax import lax
from jax.experimental import pallas as pl
from jax.experimental.pallas import tpu as pltpu
from jax.sharding import PartitionSpec as P

GRID_W = 64
EPS = 1e-06
NEG = -1e30
MESH = pl.DeviceIdType.MESH
HEADS = 12
HD = 128
ROWS = 8
PLANE = 16
SEQ = 64
LOG2E = 1.4426950408889634


def at(x, z, y):
    return x * 16 + z * 4 + y


OWNERS = (
    [at(0, 0, 0), at(1, 0, 0), at(0, 0, 1), at(0, 1, 0), at(3, 0, 0), at(1, 0, 1),
     at(0, 0, 2), at(2, 0, 0), at(1, 1, 0), at(2, 0, 1), at(0, 1, 1), at(0, 0, 3)],
    [at(3, 0, 1), at(1, 0, 2), at(1, 0, 3), at(2, 1, 0), at(2, 0, 2), at(3, 1, 0),
     at(0, 1, 2), at(1, 1, 1), at(0, 1, 3), at(2, 1, 1), at(1, 1, 2), at(3, 1, 1)],
)
HOME = set(OWNERS[1])


def ring(a):
    return min(a, 4 - a)


FAR_FIRST = sorted([(t // 16, t // 4 % 4, t % 4) for t in range(1, SEQ)], key=lambda d: -sum(map(ring, d)))


def normed(x, gain):
    mean_square = jnp.mean(x * x, axis=-1, keepdims=True)
    return x * lax.rsqrt(mean_square + EPS) * gain


def lanes():
    lane = lax.broadcasted_iota(jnp.int32, (ROWS, HD), 1)
    pair = lane >> 1
    first = pair < 8
    second = pair < 36
    within = jnp.where(first, pair, jnp.where(second, pair - 8, pair - 36)).astype(jnp.float32)
    width = jnp.where(first, 16.0, 56.0).astype(jnp.float32)
    frequency = jnp.exp(within / width * jnp.float32(-2.0 * 9.210340371976184))
    return frequency, first, second, (lane & 1) == 0


def rotary(order_ref, frequency, first, second, even):
    row = lax.broadcasted_iota(jnp.int32, (ROWS, HD), 0)
    position = jnp.zeros((ROWS, HD), jnp.int32)
    for r in range(ROWS):
        position = jnp.where(row == r, order_ref[r], position)
    half = 4 * GRID_W
    inside = position & (half - 1)
    place = jnp.where(first, position >> 8, jnp.where(second, inside >> 6, inside & (GRID_W - 1)))
    angle = place.astype(jnp.float32) * frequency
    sine = jnp.sin(angle)
    return jnp.cos(angle), jnp.where(even, -sine, sine)


def swap(x, even):
    return jnp.where(even, pltpu.roll(x, HD - 1, 1), pltpu.roll(x, 1, 1))


def turn(x, gain, cosine, sine, even):
    gains = jnp.broadcast_to(gain, x.shape)
    same, other = gains * cosine, swap(gains, even) * sine
    scale = lax.rsqrt(jnp.mean(x * x, axis=-1, keepdims=True) + EPS)
    return (x * same + swap(x, even) * other) * scale


def wide(column):
    return jnp.broadcast_to(column, (column.shape[0], HD))


def across(block, like):
    return jnp.concatenate([block] * (like.shape[1] // HD), axis=1)


def dot(a, b):
    return jnp.dot(a, b, preferred_element_type=jnp.float32)


def kernel(order_hbm, length_hbm, iq_hbm, ik_hbm, iv_hbm, tq_hbm, tk_hbm, tv_hbm,
           iq_gain_hbm, ik_gain_hbm, tq_gain_hbm, tk_gain_hbm,
           o_in,
           order, length, iq, ik, iv, tq, tk, tv, gains, kv_out, q_out, kv_in, q_in, keys, values, o_out, length_out, length_in,
           feed_send, feed_recv, load_sem, kv_send, kv_recv, q_send, q_recv, o_send, o_recv):
    loads = [
        pltpu.make_async_copy(order_hbm, order, load_sem.at[0]),
        pltpu.make_async_copy(ik_hbm, ik, load_sem.at[1]),
        pltpu.make_async_copy(ik_gain_hbm, gains.at[1:2], load_sem.at[2]),
        pltpu.make_async_copy(iv_hbm, iv, load_sem.at[3]),
        pltpu.make_async_copy(iq_hbm, iq, load_sem.at[4]),
        pltpu.make_async_copy(iq_gain_hbm, gains.at[0:1], load_sem.at[5]),
    ]
    for load in loads:
        load.start()
    me, request = lax.axis_index("seq"), lax.axis_index("req")
    x, z, y = me // 16, (me // 4) % 4, me % 4
    spot = z * 16 + x * 4 + y
    owners = [jnp.where(request == 1, b, a) for a, b in zip(*OWNERS)]
    head = jnp.int32(0)
    chip_first = me == OWNERS[0][0]
    chip_second = me == OWNERS[1][0]
    for h in range(1, HEADS):
        first, second = me == OWNERS[0][h], me == OWNERS[1][h]
        head = jnp.where(jnp.logical_or(first, second), h, head)
        chip_first, chip_second = jnp.logical_or(chip_first, first), jnp.logical_or(chip_second, second)
    feeder = jnp.logical_and(request == 0, chip_first)
    guest = jnp.logical_and(request == 1, chip_first)
    home = jnp.logical_and(request == 1, chip_second)
    owner = jnp.logical_or(guest, home)
    served = jnp.where(guest, 0, 1)
    scale = HD ** -0.5 * LOG2E

    barrier = pltpu.get_barrier_semaphore()
    column = pl.ds(pl.multiple_of(head * HD, HD), HD)
    length_load = pltpu.make_async_copy(length_hbm, length, load_sem.at[11])
    gain_loads = [
        pltpu.make_async_copy(tk_gain_hbm, gains.at[3:4], load_sem.at[6]),
        pltpu.make_async_copy(tq_gain_hbm, gains.at[2:3], load_sem.at[8]),
    ]
    text_loads = [
        pltpu.make_async_copy(tk_hbm.at[:, column], tk, load_sem.at[7]),
        pltpu.make_async_copy(tq_hbm.at[:, column], tq, load_sem.at[9]),
        pltpu.make_async_copy(tv_hbm.at[:, column], tv, load_sem.at[10]),
    ]

    @pl.when(owner)
    def _():
        with jax.named_scope("b_greet"):
            xs = [(x + d) % 4 * 16 for d in range(4)]
            zs = [(z + d) % 4 * 4 for d in range(4)]
            ys = [(y + d) % 4 for d in range(4)]
            for dx, dz, dy in FAR_FIRST:
                pl.semaphore_signal(
                    barrier, inc=1, device_id={"req": served, "seq": xs[dx] + zs[dz] + ys[dy]}, device_id_type=MESH)

            @pl.when(guest)
            def _():
                pl.semaphore_signal(barrier, inc=1, device_id={"req": 0, "seq": me}, device_id_type=MESH)

        for load in gain_loads:
            load.start()

    @pl.when(home)
    def _():
        length_load.start()
        for load in text_loads:
            load.start()

    @pl.when(feeder)
    def _():
        length_load.start()

    frequency, first, second, even = lanes()
    with jax.named_scope("c_loads"):
        for load in loads[:4]:
            load.wait()
    with jax.named_scope("e_kv"):
        cosine, sine = rotary(order, frequency, first, second, even)
        for h in range(HEADS):
            cols = slice(h * HD, (h + 1) * HD)
            k = turn(ik[:, cols].astype(jnp.float32), gains[1:2, :], cosine, sine, even)
            v = iv[:, cols].astype(jnp.float32)
            kv_out[h] = jnp.concatenate([k, v], axis=0).astype(jnp.bfloat16)

    with jax.named_scope("f_barrier"):
        @pl.when(home)
        def _():
            pl.semaphore_wait(barrier, HEADS - 1)

        @pl.when(jnp.logical_not(home))
        def _():
            pl.semaphore_wait(barrier, HEADS)

    for h in range(HEADS):
        @pl.when(jnp.logical_or(request == 0, me != owners[h]))
        def _():
            pltpu.make_async_remote_copy(
                src_ref=kv_out.at[h], dst_ref=kv_in.at[spot], send_sem=kv_send, recv_sem=kv_recv.at[z],
                device_id={"req": 1, "seq": owners[h]}, device_id_type=MESH).start()

    for load in loads[4:]:
        load.wait()
    for h in range(HEADS):
        cols = slice(h * HD, (h + 1) * HD)
        q = turn(iq[:, cols].astype(jnp.float32), gains[0:1, :], cosine, sine, even)
        q_out[h] = q.astype(jnp.bfloat16)
    for h in range(HEADS):
        @pl.when(jnp.logical_or(request == 0, me != owners[h]))
        def _():
            pltpu.make_async_remote_copy(
                src_ref=q_out.at[h], dst_ref=q_in.at[spot], send_sem=q_send, recv_sem=q_recv.at[z],
                device_id={"req": 1, "seq": owners[h]}, device_id_type=MESH).start()

    def feed(i, source, target):
        return pltpu.make_async_remote_copy(
            src_ref=source, dst_ref=target, send_sem=feed_send.at[i], recv_sem=feed_recv.at[i],
            device_id={"req": 1, "seq": me}, device_id_type=MESH)

    feeds = [
        feed(0, tk_hbm.at[:, column], tk), feed(1, tq_hbm.at[:, column], tq), feed(2, tv_hbm.at[:, column], tv),
        feed(3, length_out, length_in)]

    @pl.when(feeder)
    def _():
        for copy in feeds[:3]:
            copy.start()
        length_load.wait()
        length_out[...] = jnp.full(length_out.shape, length[0], jnp.int32)
        feeds[3].start()

    def drain(ref, count, sem):
        pltpu.make_async_copy(ref.at[pl.ds(0, count)], ref.at[pl.ds(0, count)], sem).wait()

    def arrived(ref, sem, group):
        own = jnp.logical_and(home, z == group)

        @pl.when(own)
        def _():
            drain(ref, PLANE - 1, sem.at[group])

        @pl.when(jnp.logical_not(own))
        def _():
            drain(ref, PLANE, sem.at[group])

    @pl.when(owner)
    def _():
        @pl.when(home)
        def _():
            kv_in[spot] = kv_out[head]
            q_in[spot] = q_out[head]
            length_load.wait()
            length_in[...] = jnp.full(length_in.shape, length[0], jnp.int32)
            for load in text_loads:
                load.wait()

        with jax.named_scope("j_feed"):
            @pl.when(guest)
            def _():
                for copy in feeds:
                    copy.wait_recv()

        for load in gain_loads:
            load.wait()
        with jax.named_scope("j_text"):
            text_keys = normed(tk[...].astype(jnp.float32), gains[3:4, :]).T.astype(jnp.bfloat16)
            text_values = tv[...]
            keys_in = lax.broadcasted_iota(jnp.int32, (1, text_keys.shape[1]), 1)
            valid = keys_in < across(length_in[0:1, :], keys_in)

            def text_part(q):
                s = jnp.where(valid, dot(q, text_keys), NEG)
                top = wide(jnp.max(s, axis=-1, keepdims=True))
                e = jnp.exp2((s - across(top, s)) * scale)
                total = wide(jnp.sum(e, axis=-1, keepdims=True))
                return top, total, dot(e.astype(jnp.bfloat16), text_values)

            half = PLANE * ROWS
            text_queries, text_state = {}, {}
            for group in range(4):
                rows = jnp.concatenate(
                    [tq[pl.ds(i * half + group * 32, 32), :] for i in range(4)], axis=0).astype(jnp.float32)
                text_queries[group] = normed(rows, gains[2:3, :]).astype(jnp.bfloat16)

        def both_parts(first, second):
            parts = text_part(jnp.concatenate([first, second], axis=0))
            return tuple(part[:half] for part in parts), tuple(part[half:] for part in parts)

        def image_queries(group):
            return q_in[pl.ds(group * PLANE, PLANE)].astype(jnp.float32).reshape(half, HD).astype(jnp.bfloat16)

        image_q, image_state = {}, {}
        with jax.named_scope("j_part"):
            for a, b in ((0, 1), (2, 3)):
                text_state[a], text_state[b] = both_parts(text_queries[a], text_queries[b])

        def image_part(a, b):
            for group in (a, b):
                image_q[group] = image_queries(group)
            image_state[a], image_state[b] = both_parts(image_q[a], image_q[b])

        def take_keys(group):
            arrived(kv_in, kv_recv, group)
            kv = kv_in[pl.ds(group * PLANE, PLANE)].astype(jnp.float32)
            rows = pl.ds(group * half, half)
            keys[:, rows] = kv[:, :ROWS, :].reshape(half, HD).T.astype(jnp.bfloat16)
            values[rows, :] = kv[:, ROWS:, :].reshape(half, HD).astype(jnp.bfloat16)

        with jax.named_scope("k_q"):
            arrived(q_in, q_recv, 0)
            arrived(q_in, q_recv, 1)
        with jax.named_scope("k_text"):
            image_part(0, 1)
        with jax.named_scope("l_kv"):
            for group in (0, 1, 2, 3):
                take_keys(group)
        for group in (0, 1, 2, 3):
            if group == 2:
                with jax.named_scope("l_q"):
                    arrived(q_in, q_recv, 2)
                    arrived(q_in, q_recv, 3)
                with jax.named_scope("m_text"):
                    image_part(2, 3)
            with jax.named_scope("n%d_image" % group):
                q = jnp.concatenate([image_q[group], text_queries[group]], axis=0)
                text_max, text_sum, text_out = (
                    jnp.concatenate(part, axis=0) for part in zip(image_state[group], text_state[group]))
                s = dot(q, keys[...])
                top = jnp.maximum(wide(jnp.max(s, axis=-1, keepdims=True)), text_max)
                e = jnp.exp2((s - across(top, s)) * scale)
                keep = jnp.exp2((text_max - top) * scale)
                total = wide(jnp.sum(e, axis=-1, keepdims=True)) + text_sum * keep
                o = dot(e.astype(jnp.bfloat16), values[...]) + text_out * keep
                o = o / total
                image, text = o[:half].reshape(PLANE, ROWS, HD), o[half:].reshape(PLANE, ROWS, HD)
                o_out[pl.ds(group * PLANE, PLANE)] = jnp.concatenate([image, text], axis=1).astype(jnp.bfloat16)
            with jax.named_scope("n%d_send" % group):
                for i in range(PLANE):
                    to = at(i // 4, group, i % 4)

                    def send():
                        pltpu.make_async_remote_copy(
                            src_ref=o_out.at[group * PLANE + i], dst_ref=o_in.at[head], send_sem=o_send,
                            recv_sem=o_recv, device_id={"req": served, "seq": to}, device_id_type=MESH).start()

                    if to in HOME:
                        pl.when(jnp.logical_or(guest, me != to))(send)
                    else:
                        send()
        @pl.when(home)
        def _():
            o_in[head] = o_out[spot]
            drain(o_out, SEQ - 1, o_send)

        @pl.when(guest)
        def _():
            drain(o_out, SEQ, o_send)

    @pl.when(feeder)
    def _():
        for copy in feeds:
            copy.wait_send()

    @pl.when(home)
    def _():
        drain(kv_out, HEADS - 1, kv_send)
        drain(q_out, HEADS - 1, q_send)
        with jax.named_scope("o_wait"):
            drain(o_in, HEADS - 1, o_recv)

    @pl.when(jnp.logical_not(home))
    def _():
        drain(kv_out, HEADS, kv_send)
        drain(q_out, HEADS, q_send)
        with jax.named_scope("p_wait"):
            drain(o_in, HEADS, o_recv)


def spread(o_in, image_hbm, text_hbm, image, text, sem):
    for h in range(HEADS):
        o = o_in[h].astype(jnp.float32)
        cols = slice(h * HD, (h + 1) * HD)
        image[:, cols] = o[:ROWS].astype(jnp.bfloat16)
        text[:, cols] = o[ROWS:].astype(jnp.bfloat16)
    stores = [pltpu.make_async_copy(image, image_hbm, sem.at[0]), pltpu.make_async_copy(text, text_hbm, sem.at[1])]
    for store in stores:
        store.start()
    for store in stores:
        store.wait()


def local(image_query, image_key, image_value, text_query, text_key, text_value, image_query_gain,
          image_key_gain, text_query_gain, text_key_gain, image_order, text_length):
    hbm = pl.BlockSpec(memory_space=pl.ANY)
    vmem = pl.BlockSpec(memory_space=pltpu.VMEM)
    bf16, f32 = jnp.bfloat16, jnp.float32
    width = image_query.shape[1]
    text_rows = text_key.shape[0]
    dma = pltpu.SemaphoreType.DMA
    gains = [g.reshape(1, HD) for g in (image_query_gain, image_key_gain, text_query_gain, text_key_gain)]
    blocks = pl.pallas_call(
        kernel,
        out_shape=pltpu.VMEM((HEADS, 2 * ROWS, HD), bf16),
        in_specs=[hbm] * 12,
        out_specs=vmem,
        scratch_shapes=[
            pltpu.SMEM((ROWS,), jnp.int32),
            pltpu.SMEM((1,), jnp.int32),
            pltpu.VMEM((ROWS, width), bf16),
            pltpu.VMEM((ROWS, width), bf16),
            pltpu.VMEM((ROWS, width), bf16),
            pltpu.VMEM((text_rows, HD), bf16),
            pltpu.VMEM((text_rows, HD), bf16),
            pltpu.VMEM((text_rows, HD), bf16),
            pltpu.VMEM((4, HD), f32),
            pltpu.VMEM((HEADS, 2 * ROWS, HD), bf16),
            pltpu.VMEM((HEADS, ROWS, HD), bf16),
            pltpu.VMEM((SEQ, 2 * ROWS, HD), bf16),
            pltpu.VMEM((SEQ, ROWS, HD), bf16),
            pltpu.VMEM((HD, SEQ * ROWS), bf16),
            pltpu.VMEM((SEQ * ROWS, HD), bf16),
            pltpu.VMEM((SEQ, 2 * ROWS, HD), bf16),
            pltpu.VMEM((ROWS, HD), jnp.int32),
            pltpu.VMEM((ROWS, HD), jnp.int32),
            dma((4,)), dma((4,)), dma((12,)), dma, dma((4,)), dma, dma((4,)), dma, dma,
        ],
        compiler_params=pltpu.CompilerParams(collective_id=0, has_side_effects=True),
        name="joint",
    )(image_order, text_length, image_query, image_key, image_value, text_query, text_key, text_value, *gains)
    out = jax.ShapeDtypeStruct((ROWS, width), bf16)
    return pl.pallas_call(
        spread,
        out_shape=(out, out),
        in_specs=[vmem],
        out_specs=(hbm, hbm),
        scratch_shapes=[pltpu.VMEM((ROWS, width), bf16), pltpu.VMEM((ROWS, width), bf16), dma((2,))],
        name="spread",
    )(pltpu.with_memory_space_constraint(blocks, pltpu.VMEM))


def solution(mesh):
    placed = (
        P(("req", "seq"), None),
        P(("req", "seq"), None),
        P(("req", "seq"), None),
        P("req", None),
        P("req", None),
        P("req", None),
        P(),
        P(),
        P(),
        P(),
        P(("req", "seq")),
        P("req"),
    )
    return jax.shard_map(
        local,
        mesh=mesh,
        in_specs=placed,
        out_specs=(P(("req", "seq"), None), P(("req", "seq"), None)),
        check_vma=False,
    )
```

```python
import jax
import jax.numpy as jnp
from jax import lax
from jax.experimental import pallas as pl
from jax.experimental.pallas import tpu as pltpu
from jax.sharding import PartitionSpec as P

GRID_W = 64
EPS = 1e-06
NEG = -1e30
MESH = pl.DeviceIdType.MESH
HEADS = 12
HD = 128
ROWS = 8
PLANE = 16
SEQ = 64
LOG2E = 1.4426950408889634


def at(x, z, y):
    return x * 16 + z * 4 + y


OWNERS = (
    [at(0, 0, 0), at(1, 0, 0), at(0, 0, 1), at(0, 1, 0), at(3, 0, 0), at(1, 0, 1),
     at(0, 0, 2), at(2, 0, 0), at(1, 1, 0), at(2, 0, 1), at(0, 1, 1), at(0, 0, 3)],
    [at(3, 0, 1), at(1, 0, 2), at(1, 0, 3), at(2, 1, 0), at(2, 0, 2), at(3, 1, 0),
     at(0, 1, 2), at(1, 1, 1), at(0, 1, 3), at(2, 0, 3), at(1, 1, 2), at(0, 3, 0)],
)
HOME = set(OWNERS[1])


def ring(a):
    return min(a, 4 - a)


FAR_FIRST = sorted([(t // 16, t // 4 % 4, t % 4) for t in range(1, SEQ)], key=lambda d: -sum(map(ring, d)))


def normed(x, gain):
    mean_square = jnp.mean(x * x, axis=-1, keepdims=True)
    return x * lax.rsqrt(mean_square + EPS) * gain


def lanes():
    lane = lax.broadcasted_iota(jnp.int32, (ROWS, HD), 1)
    pair = lane >> 1
    first = pair < 8
    second = pair < 36
    within = jnp.where(first, pair, jnp.where(second, pair - 8, pair - 36)).astype(jnp.float32)
    width = jnp.where(first, 16.0, 56.0).astype(jnp.float32)
    frequency = jnp.exp(within / width * jnp.float32(-2.0 * 9.210340371976184))
    return frequency, first, second, (lane & 1) == 0


def rotary(order_ref, frequency, first, second, even):
    row = lax.broadcasted_iota(jnp.int32, (ROWS, HD), 0)
    position = jnp.zeros((ROWS, HD), jnp.int32)
    for r in range(ROWS):
        position = jnp.where(row == r, order_ref[r], position)
    half = 4 * GRID_W
    inside = position & (half - 1)
    place = jnp.where(first, position >> 8, jnp.where(second, inside >> 6, inside & (GRID_W - 1)))
    angle = place.astype(jnp.float32) * frequency
    sine = jnp.sin(angle)
    return jnp.cos(angle), jnp.where(even, -sine, sine)


def swap(x, even):
    return jnp.where(even, pltpu.roll(x, HD - 1, 1), pltpu.roll(x, 1, 1))


def turn(x, gain, cosine, sine, even):
    gains = jnp.broadcast_to(gain, x.shape)
    same, other = gains * cosine, swap(gains, even) * sine
    scale = lax.rsqrt(jnp.mean(x * x, axis=-1, keepdims=True) + EPS)
    return (x * same + swap(x, even) * other) * scale


def wide(column):
    return jnp.broadcast_to(column, (column.shape[0], HD))


def across(block, like):
    return jnp.concatenate([block] * (like.shape[1] // HD), axis=1)


def dot(a, b):
    return jnp.dot(a, b, preferred_element_type=jnp.float32)


def kernel(order_hbm, length_hbm, iq_hbm, ik_hbm, iv_hbm, tq_hbm, tk_hbm, tv_hbm,
           iq_gain_hbm, ik_gain_hbm, tq_gain_hbm, tk_gain_hbm,
           o_in,
           order, length, rows_in, text_in, gains, kv_out, q_out, kv_in, q_in, keys, values, o_out, length_out, length_in,
           order_sem, rows_sem, gain_sem, text_sem, length_sem, send_sem, kv_recv, q_recv, o_send, o_recv):
    ik, iv, iq = rows_in.at[0], rows_in.at[1], rows_in.at[2]
    tk, tv, tq = text_in.at[0], text_in.at[1], text_in.at[2]
    loads = [pltpu.make_async_copy(order_hbm, order, order_sem)]
    loads += [pltpu.make_async_copy(a, b, rows_sem) for a, b in ((ik_hbm, ik), (iv_hbm, iv), (iq_hbm, iq))]
    loads += [
        pltpu.make_async_copy(a, gains.at[i:i + 1], gain_sem)
        for i, a in enumerate((iq_gain_hbm, ik_gain_hbm, tq_gain_hbm, tk_gain_hbm))]
    for load in loads:
        load.start()
    me, request = lax.axis_index("seq"), lax.axis_index("req")
    x, z, y = me // 16, (me // 4) % 4, me % 4
    spot = z * 16 + x * 4 + y
    owners = [jnp.where(request == 1, b, a) for a, b in zip(*OWNERS)]
    head = jnp.int32(0)
    chip_first = me == OWNERS[0][0]
    chip_second = me == OWNERS[1][0]
    for h in range(1, HEADS):
        first, second = me == OWNERS[0][h], me == OWNERS[1][h]
        head = jnp.where(jnp.logical_or(first, second), h, head)
        chip_first, chip_second = jnp.logical_or(chip_first, first), jnp.logical_or(chip_second, second)
    feeder = jnp.logical_and(request == 0, chip_first)
    guest = jnp.logical_and(request == 1, chip_first)
    home = jnp.logical_and(request == 1, chip_second)
    owner = jnp.logical_or(guest, home)
    served = jnp.where(guest, 0, 1)
    scale = HD ** -0.5 * LOG2E

    barrier = pltpu.get_barrier_semaphore()
    column = pl.ds(pl.multiple_of(head * HD, HD), HD)
    length_load = pltpu.make_async_copy(length_hbm, length, length_sem)
    text_slices = [(tk_hbm.at[:, column], tk), (tv_hbm.at[:, column], tv), (tq_hbm.at[:, column], tq)]

    @pl.when(owner)
    def _():
        with jax.named_scope("b_greet"):
            xs = [(x + d) % 4 * 16 for d in range(4)]
            zs = [(z + d) % 4 * 4 for d in range(4)]
            ys = [(y + d) % 4 for d in range(4)]
            for dx, dz, dy in FAR_FIRST:
                pl.semaphore_signal(
                    barrier, inc=1, device_id={"req": served, "seq": xs[dx] + zs[dz] + ys[dy]}, device_id_type=MESH)

            @pl.when(guest)
            def _():
                pl.semaphore_signal(barrier, inc=1, device_id={"req": 0, "seq": me}, device_id_type=MESH)

    @pl.when(home)
    def _():
        length_load.start()
        for source, target in text_slices:
            pltpu.make_async_copy(source, target, text_sem).start()

    @pl.when(feeder)
    def _():
        length_load.start()

    frequency, first, second, even = lanes()
    def settle(ref, sem):
        pltpu.make_async_copy(ref, ref, sem).wait()

    with jax.named_scope("c_loads"):
        loads[0].wait()
        settle(gains, gain_sem)
        settle(rows_in, rows_sem)
    with jax.named_scope("e_kv"):
        cosine, sine = rotary(order, frequency, first, second, even)
        for h in range(HEADS):
            cols = slice(h * HD, (h + 1) * HD)
            k = turn(ik[:, cols].astype(jnp.float32), gains[1:2, :], cosine, sine, even)
            v = iv[:, cols].astype(jnp.float32)
            kv_out[h] = jnp.concatenate([k, v], axis=0).astype(jnp.bfloat16)

    with jax.named_scope("f_barrier"):
        @pl.when(home)
        def _():
            pl.semaphore_wait(barrier, HEADS - 1)

        @pl.when(jnp.logical_not(home))
        def _():
            pl.semaphore_wait(barrier, HEADS)

    for h in range(HEADS):
        @pl.when(jnp.logical_or(request == 0, me != owners[h]))
        def _():
            pltpu.make_async_remote_copy(
                src_ref=kv_out.at[h], dst_ref=kv_in.at[spot], send_sem=send_sem, recv_sem=kv_recv,
                device_id={"req": 1, "seq": owners[h]}, device_id_type=MESH).start()

    for h in range(HEADS):
        cols = slice(h * HD, (h + 1) * HD)
        q = turn(iq[:, cols].astype(jnp.float32), gains[0:1, :], cosine, sine, even)
        q_out[h] = q.astype(jnp.bfloat16)
    for h in range(HEADS):
        @pl.when(jnp.logical_or(request == 0, me != owners[h]))
        def _():
            pltpu.make_async_remote_copy(
                src_ref=q_out.at[h], dst_ref=q_in.at[spot], send_sem=send_sem, recv_sem=q_recv.at[z // 2],
                device_id={"req": 1, "seq": owners[h]}, device_id_type=MESH).start()

    def feed(source, target, sem):
        return pltpu.make_async_remote_copy(
            src_ref=source, dst_ref=target, send_sem=sem, recv_sem=sem, device_id={"req": 1, "seq": me},
            device_id_type=MESH)

    @pl.when(feeder)
    def _():
        for source, target in text_slices:
            feed(source, target, text_sem).start()
        length_load.wait()
        length_out[...] = jnp.full(length_out.shape, length[0], jnp.int32)
        feed(length_out, length_in, length_sem).start()

    def drain(ref, count, sem):
        settle(ref.at[pl.ds(0, count)], sem)

    def arrived(ref, count, sem, own):
        @pl.when(own)
        def _():
            drain(ref, count - 1, sem)

        @pl.when(jnp.logical_not(own))
        def _():
            drain(ref, count, sem)

    def queries_arrived(pair):
        arrived(q_in, 2 * PLANE, q_recv.at[pair], jnp.logical_and(home, z // 2 == pair))

    @pl.when(owner)
    def _():
        @pl.when(home)
        def _():
            kv_in[spot] = kv_out[head]
            q_in[spot] = q_out[head]
            length_load.wait()
            length_in[...] = jnp.full(length_in.shape, length[0], jnp.int32)

        with jax.named_scope("j_feed"):
            settle(text_in, text_sem)

            @pl.when(guest)
            def _():
                settle(length_in, length_sem)

        with jax.named_scope("j_text"):
            text_keys = normed(tk[...].astype(jnp.float32), gains[3:4, :]).T.astype(jnp.bfloat16)
            text_values = tv[...]
            keys_in = lax.broadcasted_iota(jnp.int32, (1, text_keys.shape[1]), 1)
            valid = keys_in < across(length_in[0:1, :], keys_in)

            def text_part(q):
                s = jnp.where(valid, dot(q, text_keys), NEG)
                top = wide(jnp.max(s, axis=-1, keepdims=True))
                e = jnp.exp2((s - across(top, s)) * scale)
                total = wide(jnp.sum(e, axis=-1, keepdims=True))
                return top, total, dot(e.astype(jnp.bfloat16), text_values)

            half = PLANE * ROWS
            text_queries, text_state = {}, {}
            for group in range(4):
                rows = jnp.concatenate(
                    [tq[pl.ds(i * half + group * 32, 32), :] for i in range(4)], axis=0).astype(jnp.float32)
                text_queries[group] = normed(rows, gains[2:3, :]).astype(jnp.bfloat16)

        def both_parts(first, second):
            parts = text_part(jnp.concatenate([first, second], axis=0))
            return tuple(part[:half] for part in parts), tuple(part[half:] for part in parts)

        def image_queries(group):
            return q_in[pl.ds(group * PLANE, PLANE)].astype(jnp.float32).reshape(half, HD).astype(jnp.bfloat16)

        image_q, image_state = {}, {}
        with jax.named_scope("j_part"):
            for a, b in ((0, 1), (2, 3)):
                text_state[a], text_state[b] = both_parts(text_queries[a], text_queries[b])

        def image_part(a, b):
            for group in (a, b):
                image_q[group] = image_queries(group)
            image_state[a], image_state[b] = both_parts(image_q[a], image_q[b])

        with jax.named_scope("k_q"):
            queries_arrived(0)
        with jax.named_scope("k_text"):
            image_part(0, 1)
        with jax.named_scope("l_kv"):
            arrived(kv_in, SEQ, kv_recv, home)
        kv = kv_in[...].astype(jnp.float32)
        keys[...] = kv[:, :ROWS, :].reshape(SEQ * ROWS, HD).astype(jnp.bfloat16)
        values[...] = kv[:, ROWS:, :].reshape(SEQ * ROWS, HD).astype(jnp.bfloat16)
        for group in (0, 1, 2, 3):
            if group == 2:
                with jax.named_scope("l_q"):
                    queries_arrived(1)
                with jax.named_scope("m_text"):
                    image_part(2, 3)
            with jax.named_scope("n%d_image" % group):
                q = jnp.concatenate([image_q[group], text_queries[group]], axis=0)
                text_max, text_sum, text_out = (
                    jnp.concatenate(part, axis=0) for part in zip(image_state[group], text_state[group]))
                s = lax.dot_general(
                    q, keys[...], (((1,), (1,)), ((), ())), preferred_element_type=jnp.float32)
                top = jnp.maximum(wide(jnp.max(s, axis=-1, keepdims=True)), text_max)
                e = jnp.exp2((s - across(top, s)) * scale)
                keep = jnp.exp2((text_max - top) * scale)
                total = wide(jnp.sum(e, axis=-1, keepdims=True)) + text_sum * keep
                o = dot(e.astype(jnp.bfloat16), values[...]) + text_out * keep
                o = o / total
                image, text = o[:half].reshape(PLANE, ROWS, HD), o[half:].reshape(PLANE, ROWS, HD)
                o_out[pl.ds(group * PLANE, PLANE)] = jnp.concatenate([image, text], axis=1).astype(jnp.bfloat16)
            with jax.named_scope("n%d_send" % group):
                for i in range(PLANE):
                    to = at(i // 4, group, i % 4)

                    def send():
                        pltpu.make_async_remote_copy(
                            src_ref=o_out.at[group * PLANE + i], dst_ref=o_in.at[head], send_sem=o_send,
                            recv_sem=o_recv, device_id={"req": served, "seq": to}, device_id_type=MESH).start()

                    if to in HOME:
                        pl.when(jnp.logical_or(guest, me != to))(send)
                    else:
                        send()
        @pl.when(home)
        def _():
            o_in[head] = o_out[spot]
            drain(o_out, SEQ - 1, o_send)

        @pl.when(guest)
        def _():
            drain(o_out, SEQ, o_send)

    @pl.when(feeder)
    def _():
        settle(text_in, text_sem)
        settle(length_out, length_sem)

    @pl.when(home)
    def _():
        drain(q_in, 3 * (HEADS - 1), send_sem)
        with jax.named_scope("o_wait"):
            drain(o_in, HEADS - 1, o_recv)

    @pl.when(jnp.logical_not(home))
    def _():
        drain(q_in, 3 * HEADS, send_sem)
        with jax.named_scope("p_wait"):
            drain(o_in, HEADS, o_recv)


def spread(o_in, image_hbm, text_hbm, image, text, sem):
    for h in range(HEADS):
        o = o_in[h].astype(jnp.float32)
        cols = slice(h * HD, (h + 1) * HD)
        image[:, cols] = o[:ROWS].astype(jnp.bfloat16)
        text[:, cols] = o[ROWS:].astype(jnp.bfloat16)
    pltpu.make_async_copy(image, image_hbm, sem).start()
    pltpu.make_async_copy(text, text_hbm, sem).start()
    pltpu.make_async_copy(o_in, o_in, sem).wait()


def local(image_query, image_key, image_value, text_query, text_key, text_value, image_query_gain,
          image_key_gain, text_query_gain, text_key_gain, image_order, text_length):
    hbm = pl.BlockSpec(memory_space=pl.ANY)
    vmem = pl.BlockSpec(memory_space=pltpu.VMEM)
    bf16, f32 = jnp.bfloat16, jnp.float32
    width = image_query.shape[1]
    text_rows = text_key.shape[0]
    dma = pltpu.SemaphoreType.DMA
    gains = [g.reshape(1, HD) for g in (image_query_gain, image_key_gain, text_query_gain, text_key_gain)]
    blocks = pl.pallas_call(
        kernel,
        out_shape=pltpu.VMEM((HEADS, 2 * ROWS, HD), bf16),
        in_specs=[hbm] * 12,
        out_specs=vmem,
        scratch_shapes=[
            pltpu.SMEM((ROWS,), jnp.int32),
            pltpu.SMEM((1,), jnp.int32),
            pltpu.VMEM((3, ROWS, width), bf16),
            pltpu.VMEM((3, text_rows, HD), bf16),
            pltpu.VMEM((4, HD), f32),
            pltpu.VMEM((HEADS, 2 * ROWS, HD), bf16),
            pltpu.VMEM((HEADS, ROWS, HD), bf16),
            pltpu.VMEM((SEQ, 2 * ROWS, HD), bf16),
            pltpu.VMEM((SEQ, ROWS, HD), bf16),
            pltpu.VMEM((SEQ * ROWS, HD), bf16),
            pltpu.VMEM((SEQ * ROWS, HD), bf16),
            pltpu.VMEM((SEQ, 2 * ROWS, HD), bf16),
            pltpu.VMEM((ROWS, HD), jnp.int32),
            pltpu.VMEM((ROWS, HD), jnp.int32),
            dma, dma, dma, dma, dma, dma, dma, dma((2,)), dma, dma,
        ],
        compiler_params=pltpu.CompilerParams(collective_id=0, has_side_effects=True),
        name="joint",
    )(image_order, text_length, image_query, image_key, image_value, text_query, text_key, text_value, *gains)
    out = jax.ShapeDtypeStruct((ROWS, width), bf16)
    return pl.pallas_call(
        spread,
        out_shape=(out, out),
        in_specs=[vmem],
        out_specs=(hbm, hbm),
        scratch_shapes=[pltpu.VMEM((ROWS, width), bf16), pltpu.VMEM((ROWS, width), bf16), dma],
        name="spread",
    )(pltpu.with_memory_space_constraint(blocks, pltpu.VMEM))


def solution(mesh):
    placed = (
        P(("req", "seq"), None),
        P(("req", "seq"), None),
        P(("req", "seq"), None),
        P("req", None),
        P("req", None),
        P("req", None),
        P(),
        P(),
        P(),
        P(),
        P(("req", "seq")),
        P("req"),
    )
    return jax.shard_map(
        local,
        mesh=mesh,
        in_specs=placed,
        out_specs=(P(("req", "seq"), None), P(("req", "seq"), None)),
        check_vma=False,
    )
```

```python
import jax
import jax.numpy as jnp
from jax import lax
from jax.experimental import pallas as pl
from jax.experimental.pallas import tpu as pltpu
from jax.sharding import PartitionSpec as P

GRID_W = 64
EPS = 1e-06
NEG = -1e30
MESH = pl.DeviceIdType.MESH
HEADS = 12
HD = 128
ROWS = 8
PLANE = 16
SEQ = 64
LOG2E = 1.4426950408889634


def at(x, z, y):
    return x * 16 + z * 4 + y


OWNERS = (
    [at(0, 0, 0), at(1, 0, 0), at(0, 0, 1), at(0, 1, 0), at(3, 0, 0), at(1, 0, 1),
     at(0, 0, 2), at(2, 0, 0), at(1, 1, 0), at(2, 0, 1), at(0, 1, 1), at(0, 0, 3)],
    [at(3, 0, 1), at(1, 0, 2), at(1, 0, 3), at(2, 1, 0), at(3, 1, 1), at(3, 1, 0),
     at(0, 1, 2), at(1, 1, 1), at(0, 1, 3), at(1, 1, 3), at(0, 2, 0), at(0, 3, 0)],
)
HOME = set(OWNERS[1])


def ring(a):
    return min(a, 4 - a)


FAR_FIRST = sorted([(t // 16, t // 4 % 4, t % 4) for t in range(1, SEQ)], key=lambda d: -sum(map(ring, d)))


def normed(x, gain):
    mean_square = jnp.mean(x * x, axis=-1, keepdims=True)
    return x * lax.rsqrt(mean_square + EPS) * gain


def lanes():
    lane = lax.broadcasted_iota(jnp.int32, (ROWS, HD), 1)
    pair = lane >> 1
    first = pair < 8
    second = pair < 36
    within = jnp.where(first, pair, jnp.where(second, pair - 8, pair - 36)).astype(jnp.float32)
    width = jnp.where(first, 16.0, 56.0).astype(jnp.float32)
    frequency = jnp.exp(within / width * jnp.float32(-2.0 * 9.210340371976184))
    return frequency, first, second, (lane & 1) == 0


def rotary(order_ref, frequency, first, second, even):
    row = lax.broadcasted_iota(jnp.int32, (ROWS, HD), 0)
    position = jnp.zeros((ROWS, HD), jnp.int32)
    for r in range(ROWS):
        position = jnp.where(row == r, order_ref[r], position)
    half = 4 * GRID_W
    inside = position & (half - 1)
    place = jnp.where(first, position >> 8, jnp.where(second, inside >> 6, inside & (GRID_W - 1)))
    angle = place.astype(jnp.float32) * frequency
    sine = jnp.sin(angle)
    return jnp.cos(angle), jnp.where(even, -sine, sine)


def swap(x, even):
    return jnp.where(even, pltpu.roll(x, HD - 1, 1), pltpu.roll(x, 1, 1))


def turn(x, gain, cosine, sine, even):
    gains = jnp.broadcast_to(gain, x.shape)
    same, other = gains * cosine, swap(gains, even) * sine
    scale = lax.rsqrt(jnp.mean(x * x, axis=-1, keepdims=True) + EPS)
    return (x * same + swap(x, even) * other) * scale


def wide(column):
    return jnp.broadcast_to(column, (column.shape[0], HD))


def across(block, like):
    return jnp.concatenate([block] * (like.shape[1] // HD), axis=1)


def dot(a, b):
    return jnp.dot(a, b, preferred_element_type=jnp.float32)


def kernel(order_hbm, length_hbm, iq_hbm, ik_hbm, iv_hbm, tq_hbm, tk_hbm, tv_hbm,
           iq_gain_hbm, ik_gain_hbm, tq_gain_hbm, tk_gain_hbm,
           o_in,
           order, length, rows_in, text_in, gains, kv_out, q_out, kv_in, q_in, keys, values, o_out, length_out, length_in,
           order_sem, rows_sem, gain_sem, text_sem, length_sem, send_sem, kv_recv, q_recv, o_send, o_recv):
    ik, iv, iq = rows_in.at[0], rows_in.at[1], rows_in.at[2]
    tk, tv, tq = text_in.at[0], text_in.at[1], text_in.at[2]
    loads = [pltpu.make_async_copy(order_hbm, order, order_sem)]
    loads += [pltpu.make_async_copy(a, b, rows_sem) for a, b in ((ik_hbm, ik), (iv_hbm, iv), (iq_hbm, iq))]
    loads += [
        pltpu.make_async_copy(a, gains.at[i:i + 1], gain_sem)
        for i, a in enumerate((iq_gain_hbm, ik_gain_hbm, tq_gain_hbm, tk_gain_hbm))]
    for load in loads:
        load.start()
    me, request = lax.axis_index("seq"), lax.axis_index("req")
    x, z, y = me // 16, (me // 4) % 4, me % 4
    spot = z * 16 + x * 4 + y
    owners = [jnp.where(request == 1, b, a) for a, b in zip(*OWNERS)]
    head = jnp.int32(0)
    chip_first = me == OWNERS[0][0]
    chip_second = me == OWNERS[1][0]
    for h in range(1, HEADS):
        first, second = me == OWNERS[0][h], me == OWNERS[1][h]
        head = jnp.where(jnp.logical_or(first, second), h, head)
        chip_first, chip_second = jnp.logical_or(chip_first, first), jnp.logical_or(chip_second, second)
    feeder = jnp.logical_and(request == 0, chip_first)
    guest = jnp.logical_and(request == 1, chip_first)
    home = jnp.logical_and(request == 1, chip_second)
    owner = jnp.logical_or(guest, home)
    served = jnp.where(guest, 0, 1)
    scale = HD ** -0.5 * LOG2E

    barrier = pltpu.get_barrier_semaphore()
    column = pl.ds(pl.multiple_of(head * HD, HD), HD)
    length_load = pltpu.make_async_copy(length_hbm, length, length_sem)
    text_slices = [(tk_hbm.at[:, column], tk), (tv_hbm.at[:, column], tv), (tq_hbm.at[:, column], tq)]

    @pl.when(owner)
    def _():
        with jax.named_scope("b_greet"):
            xs = [(x + d) % 4 * 16 for d in range(4)]
            zs = [(z + d) % 4 * 4 for d in range(4)]
            ys = [(y + d) % 4 for d in range(4)]
            for dx, dz, dy in FAR_FIRST:
                pl.semaphore_signal(
                    barrier, inc=1, device_id={"req": served, "seq": xs[dx] + zs[dz] + ys[dy]}, device_id_type=MESH)

            @pl.when(guest)
            def _():
                pl.semaphore_signal(barrier, inc=1, device_id={"req": 0, "seq": me}, device_id_type=MESH)

    @pl.when(home)
    def _():
        length_load.start()
        for source, target in text_slices:
            pltpu.make_async_copy(source, target, text_sem).start()

    @pl.when(feeder)
    def _():
        length_load.start()

    frequency, first, second, even = lanes()
    def settle(ref, sem):
        pltpu.make_async_copy(ref, ref, sem).wait()

    with jax.named_scope("c_loads"):
        loads[0].wait()
        settle(gains, gain_sem)
        settle(rows_in, rows_sem)
    with jax.named_scope("e_kv"):
        cosine, sine = rotary(order, frequency, first, second, even)
        for h in range(HEADS):
            cols = slice(h * HD, (h + 1) * HD)
            k = turn(ik[:, cols].astype(jnp.float32), gains[1:2, :], cosine, sine, even)
            v = iv[:, cols].astype(jnp.float32)
            kv_out[h] = jnp.concatenate([k, v], axis=0).astype(jnp.bfloat16)

    with jax.named_scope("f_barrier"):
        @pl.when(home)
        def _():
            pl.semaphore_wait(barrier, HEADS - 1)

        @pl.when(jnp.logical_not(home))
        def _():
            pl.semaphore_wait(barrier, HEADS)

    for h in range(HEADS):
        @pl.when(jnp.logical_or(request == 0, me != owners[h]))
        def _():
            pltpu.make_async_remote_copy(
                src_ref=kv_out.at[h], dst_ref=kv_in.at[spot], send_sem=send_sem, recv_sem=kv_recv,
                device_id={"req": 1, "seq": owners[h]}, device_id_type=MESH).start()

    for h in range(HEADS):
        cols = slice(h * HD, (h + 1) * HD)
        q = turn(iq[:, cols].astype(jnp.float32), gains[0:1, :], cosine, sine, even)
        q_out[h] = q.astype(jnp.bfloat16)
    for h in range(HEADS):
        @pl.when(jnp.logical_or(request == 0, me != owners[h]))
        def _():
            pltpu.make_async_remote_copy(
                src_ref=q_out.at[h], dst_ref=q_in.at[spot], send_sem=send_sem, recv_sem=q_recv.at[z // 2],
                device_id={"req": 1, "seq": owners[h]}, device_id_type=MESH).start()

    def feed(source, target, sem):
        return pltpu.make_async_remote_copy(
            src_ref=source, dst_ref=target, send_sem=sem, recv_sem=sem, device_id={"req": 1, "seq": me},
            device_id_type=MESH)

    @pl.when(feeder)
    def _():
        for source, target in text_slices:
            feed(source, target, text_sem).start()
        length_load.wait()
        length_out[...] = jnp.full(length_out.shape, length[0], jnp.int32)
        feed(length_out, length_in, length_sem).start()

    def drain(ref, count, sem):
        settle(ref.at[pl.ds(0, count)], sem)

    def arrived(ref, count, sem, own):
        @pl.when(own)
        def _():
            drain(ref, count - 1, sem)

        @pl.when(jnp.logical_not(own))
        def _():
            drain(ref, count, sem)

    def queries_arrived(pair):
        arrived(q_in, 2 * PLANE, q_recv.at[pair], jnp.logical_and(home, z // 2 == pair))

    @pl.when(owner)
    def _():
        @pl.when(home)
        def _():
            kv_in[spot] = kv_out[head]
            q_in[spot] = q_out[head]
            length_load.wait()
            length_in[...] = jnp.full(length_in.shape, length[0], jnp.int32)

        with jax.named_scope("j_feed"):
            settle(text_in, text_sem)

            @pl.when(guest)
            def _():
                settle(length_in, length_sem)

        with jax.named_scope("j_text"):
            text_keys = normed(tk[...].astype(jnp.float32), gains[3:4, :]).T.astype(jnp.bfloat16)
            text_values = tv[...]
            keys_in = lax.broadcasted_iota(jnp.int32, (1, text_keys.shape[1]), 1)
            valid = keys_in < across(length_in[0:1, :], keys_in)

            def text_part(q):
                s = jnp.where(valid, dot(q, text_keys), NEG)
                top = wide(jnp.max(s, axis=-1, keepdims=True))
                e = jnp.exp2((s - across(top, s)) * scale)
                total = wide(jnp.sum(e, axis=-1, keepdims=True))
                return top, total, dot(e.astype(jnp.bfloat16), text_values)

            half = PLANE * ROWS
            text_queries, text_state = {}, {}
            for group in range(4):
                rows = jnp.concatenate(
                    [tq[pl.ds(i * half + group * 32, 32), :] for i in range(4)], axis=0).astype(jnp.float32)
                text_queries[group] = normed(rows, gains[2:3, :]).astype(jnp.bfloat16)

        def both_parts(first, second):
            parts = text_part(jnp.concatenate([first, second], axis=0))
            return tuple(part[:half] for part in parts), tuple(part[half:] for part in parts)

        def image_queries(group):
            return q_in[pl.ds(group * PLANE, PLANE)].astype(jnp.float32).reshape(half, HD).astype(jnp.bfloat16)

        image_q, image_state = {}, {}
        with jax.named_scope("j_part"):
            for a, b in ((0, 1), (2, 3)):
                text_state[a], text_state[b] = both_parts(text_queries[a], text_queries[b])

        def image_part(a, b):
            for group in (a, b):
                image_q[group] = image_queries(group)
            image_state[a], image_state[b] = both_parts(image_q[a], image_q[b])

        with jax.named_scope("k_q"):
            queries_arrived(0)
        with jax.named_scope("k_text"):
            image_part(0, 1)
        with jax.named_scope("l_kv"):
            arrived(kv_in, SEQ, kv_recv, home)
        kv = kv_in[...].astype(jnp.float32)
        keys[...] = kv[:, :ROWS, :].reshape(SEQ * ROWS, HD).astype(jnp.bfloat16)
        values[...] = kv[:, ROWS:, :].reshape(SEQ * ROWS, HD).astype(jnp.bfloat16)
        for group in (0, 1, 2, 3):
            if group == 2:
                with jax.named_scope("l_q"):
                    queries_arrived(1)
                with jax.named_scope("m_text"):
                    image_part(2, 3)
            with jax.named_scope("n%d_image" % group):
                q = jnp.concatenate([image_q[group], text_queries[group]], axis=0)
                text_max, text_sum, text_out = (
                    jnp.concatenate(part, axis=0) for part in zip(image_state[group], text_state[group]))
                s = lax.dot_general(
                    q, keys[...], (((1,), (1,)), ((), ())), preferred_element_type=jnp.float32)
                top = jnp.maximum(wide(jnp.max(s, axis=-1, keepdims=True)), text_max)
                e = jnp.exp2((s - across(top, s)) * scale)
                keep = jnp.exp2((text_max - top) * scale)
                total = wide(jnp.sum(e, axis=-1, keepdims=True)) + text_sum * keep
                o = dot(e.astype(jnp.bfloat16), values[...]) + text_out * keep
                o = o / total
                image, text = o[:half].reshape(PLANE, ROWS, HD), o[half:].reshape(PLANE, ROWS, HD)
                o_out[pl.ds(group * PLANE, PLANE)] = jnp.concatenate([image, text], axis=1).astype(jnp.bfloat16)
            with jax.named_scope("n%d_send" % group):
                for i in range(PLANE):
                    to = at(i // 4, group, i % 4)

                    def send():
                        pltpu.make_async_remote_copy(
                            src_ref=o_out.at[group * PLANE + i], dst_ref=o_in.at[head], send_sem=o_send,
                            recv_sem=o_recv, device_id={"req": served, "seq": to}, device_id_type=MESH).start()

                    if to in HOME:
                        pl.when(jnp.logical_or(guest, me != to))(send)
                    else:
                        send()
        @pl.when(home)
        def _():
            o_in[head] = o_out[spot]
            drain(o_out, SEQ - 1, o_send)

        @pl.when(guest)
        def _():
            drain(o_out, SEQ, o_send)

    @pl.when(feeder)
    def _():
        settle(text_in, text_sem)
        settle(length_out, length_sem)

    @pl.when(home)
    def _():
        drain(q_in, 3 * (HEADS - 1), send_sem)
        with jax.named_scope("o_wait"):
            drain(o_in, HEADS - 1, o_recv)

    @pl.when(jnp.logical_not(home))
    def _():
        drain(q_in, 3 * HEADS, send_sem)
        with jax.named_scope("p_wait"):
            drain(o_in, HEADS, o_recv)


def spread(o_in, image_hbm, text_hbm, image, text, sem):
    for h in range(HEADS):
        o = o_in[h].astype(jnp.float32)
        cols = slice(h * HD, (h + 1) * HD)
        image[:, cols] = o[:ROWS].astype(jnp.bfloat16)
        text[:, cols] = o[ROWS:].astype(jnp.bfloat16)
    pltpu.make_async_copy(image, image_hbm, sem).start()
    pltpu.make_async_copy(text, text_hbm, sem).start()
    pltpu.make_async_copy(o_in, o_in, sem).wait()


def local(image_query, image_key, image_value, text_query, text_key, text_value, image_query_gain,
          image_key_gain, text_query_gain, text_key_gain, image_order, text_length):
    hbm = pl.BlockSpec(memory_space=pl.ANY)
    vmem = pl.BlockSpec(memory_space=pltpu.VMEM)
    bf16, f32 = jnp.bfloat16, jnp.float32
    width = image_query.shape[1]
    text_rows = text_key.shape[0]
    dma = pltpu.SemaphoreType.DMA
    gains = [g.reshape(1, HD) for g in (image_query_gain, image_key_gain, text_query_gain, text_key_gain)]
    blocks = pl.pallas_call(
        kernel,
        out_shape=pltpu.VMEM((HEADS, 2 * ROWS, HD), bf16),
        in_specs=[hbm] * 12,
        out_specs=vmem,
        scratch_shapes=[
            pltpu.SMEM((ROWS,), jnp.int32),
            pltpu.SMEM((1,), jnp.int32),
            pltpu.VMEM((3, ROWS, width), bf16),
            pltpu.VMEM((3, text_rows, HD), bf16),
            pltpu.VMEM((4, HD), f32),
            pltpu.VMEM((HEADS, 2 * ROWS, HD), bf16),
            pltpu.VMEM((HEADS, ROWS, HD), bf16),
            pltpu.VMEM((SEQ, 2 * ROWS, HD), bf16),
            pltpu.VMEM((SEQ, ROWS, HD), bf16),
            pltpu.VMEM((SEQ * ROWS, HD), bf16),
            pltpu.VMEM((SEQ * ROWS, HD), bf16),
            pltpu.VMEM((SEQ, 2 * ROWS, HD), bf16),
            pltpu.VMEM((ROWS, HD), jnp.int32),
            pltpu.VMEM((ROWS, HD), jnp.int32),
            dma, dma, dma, dma, dma, dma, dma, dma((2,)), dma, dma,
        ],
        compiler_params=pltpu.CompilerParams(collective_id=0, has_side_effects=True),
        name="joint",
    )(image_order, text_length, image_query, image_key, image_value, text_query, text_key, text_value, *gains)
    out = jax.ShapeDtypeStruct((ROWS, width), bf16)
    return pl.pallas_call(
        spread,
        out_shape=(out, out),
        in_specs=[vmem],
        out_specs=(hbm, hbm),
        scratch_shapes=[pltpu.VMEM((ROWS, width), bf16), pltpu.VMEM((ROWS, width), bf16), dma],
        name="spread",
    )(pltpu.with_memory_space_constraint(blocks, pltpu.VMEM))


def solution(mesh):
    placed = (
        P(("req", "seq"), None),
        P(("req", "seq"), None),
        P(("req", "seq"), None),
        P("req", None),
        P("req", None),
        P("req", None),
        P(),
        P(),
        P(),
        P(),
        P(("req", "seq")),
        P("req"),
    )
    return jax.shard_map(
        local,
        mesh=mesh,
        in_specs=placed,
        out_specs=(P(("req", "seq"), None), P(("req", "seq"), None)),
        check_vma=False,
    )
```

```python
import jax
import jax.numpy as jnp
from jax import lax
from jax.experimental import pallas as pl
from jax.experimental.pallas import tpu as pltpu
from jax.sharding import PartitionSpec as P

GRID_W = 64
EPS = 1e-06
NEG = -1e30
MESH = pl.DeviceIdType.MESH
HEADS = 12
HD = 128
ROWS = 8
PLANE = 16
SEQ = 64
LOG2E = 1.4426950408889634


def at(x, z, y):
    return x * 16 + z * 4 + y


OWNERS = (
    [at(0, 0, 0), at(1, 0, 0), at(0, 0, 1), at(0, 1, 0), at(3, 0, 0), at(1, 0, 1),
     at(0, 0, 2), at(2, 0, 0), at(1, 1, 0), at(2, 0, 1), at(0, 1, 1), at(0, 0, 3)],
    [at(3, 0, 1), at(1, 0, 2), at(1, 0, 3), at(2, 1, 0), at(3, 1, 1), at(3, 1, 0),
     at(0, 1, 2), at(1, 1, 1), at(0, 1, 3), at(1, 1, 3), at(0, 2, 0), at(0, 3, 0)],
)
HOME = set(OWNERS[1])


def ring(a):
    return min(a, 4 - a)


FAR_FIRST = sorted([(t // 16, t // 4 % 4, t % 4) for t in range(1, SEQ)], key=lambda d: -sum(map(ring, d)))


def normed(x, gain):
    mean_square = jnp.mean(x * x, axis=-1, keepdims=True)
    return x * lax.rsqrt(mean_square + EPS) * gain


def lanes():
    lane = lax.broadcasted_iota(jnp.int32, (ROWS, HD), 1)
    pair = lane >> 1
    first = pair < 8
    second = pair < 36
    within = jnp.where(first, pair, jnp.where(second, pair - 8, pair - 36)).astype(jnp.float32)
    width = jnp.where(first, 16.0, 56.0).astype(jnp.float32)
    frequency = jnp.exp(within / width * jnp.float32(-2.0 * 9.210340371976184))
    return frequency, first, second, (lane & 1) == 0


def rotary(order_ref, frequency, first, second, even):
    row = lax.broadcasted_iota(jnp.int32, (ROWS, HD), 0)
    position = jnp.zeros((ROWS, HD), jnp.int32)
    for r in range(ROWS):
        position = jnp.where(row == r, order_ref[r], position)
    half = 4 * GRID_W
    inside = position & (half - 1)
    place = jnp.where(first, position >> 8, jnp.where(second, inside >> 6, inside & (GRID_W - 1)))
    angle = place.astype(jnp.float32) * frequency
    sine = jnp.sin(angle)
    return jnp.cos(angle), jnp.where(even, -sine, sine)


def swap(x, even):
    return jnp.where(even, pltpu.roll(x, HD - 1, 1), pltpu.roll(x, 1, 1))


def turn(x, gain, cosine, sine, even):
    gains = jnp.broadcast_to(gain, x.shape)
    same, other = gains * cosine, swap(gains, even) * sine
    scale = lax.rsqrt(jnp.mean(x * x, axis=-1, keepdims=True) + EPS)
    return (x * same + swap(x, even) * other) * scale


def wide(column):
    return jnp.broadcast_to(column, (column.shape[0], HD))


def across(block, like):
    return jnp.concatenate([block] * (like.shape[1] // HD), axis=1)


def dot(a, b):
    return jnp.dot(a, b, preferred_element_type=jnp.float32)


def kernel(order_hbm, length_hbm, iq_hbm, ik_hbm, iv_hbm, tq_hbm, tk_hbm, tv_hbm,
           iq_gain_hbm, ik_gain_hbm, tq_gain_hbm, tk_gain_hbm,
           o_in,
           order, length, rows_in, text_in, gains, kv_out, q_out, kv_in, q_in, keys, values, o_out, length_out, length_in,
           order_sem, rows_sem, gain_sem, text_sem, length_sem, send_sem, kv_recv, q_recv, o_send, o_recv):
    ik, iv, iq = rows_in.at[0], rows_in.at[1], rows_in.at[2]
    tk, tv, tq = text_in.at[0], text_in.at[1], text_in.at[2]
    loads = [pltpu.make_async_copy(order_hbm, order, order_sem)]
    loads += [pltpu.make_async_copy(a, b, rows_sem) for a, b in ((ik_hbm, ik), (iv_hbm, iv), (iq_hbm, iq))]
    loads += [
        pltpu.make_async_copy(a, gains.at[i:i + 1], gain_sem)
        for i, a in enumerate((iq_gain_hbm, ik_gain_hbm, tq_gain_hbm, tk_gain_hbm))]
    for load in loads:
        load.start()
    me, request = lax.axis_index("seq"), lax.axis_index("req")
    x, z, y = me // 16, (me // 4) % 4, me % 4
    spot = z * 16 + x * 4 + y
    owners = [jnp.where(request == 1, b, a) for a, b in zip(*OWNERS)]
    head = jnp.int32(0)
    chip_first = me == OWNERS[0][0]
    chip_second = me == OWNERS[1][0]
    for h in range(1, HEADS):
        first, second = me == OWNERS[0][h], me == OWNERS[1][h]
        head = jnp.where(jnp.logical_or(first, second), h, head)
        chip_first, chip_second = jnp.logical_or(chip_first, first), jnp.logical_or(chip_second, second)
    feeder = jnp.logical_and(request == 0, chip_first)
    guest = jnp.logical_and(request == 1, chip_first)
    home = jnp.logical_and(request == 1, chip_second)
    owner = jnp.logical_or(guest, home)
    served = jnp.where(guest, 0, 1)
    scale = HD ** -0.5 * LOG2E

    barrier = pltpu.get_barrier_semaphore()
    column = pl.ds(pl.multiple_of(head * HD, HD), HD)
    length_load = pltpu.make_async_copy(length_hbm, length, length_sem)
    text_slices = [(tk_hbm.at[:, column], tk), (tv_hbm.at[:, column], tv), (tq_hbm.at[:, column], tq)]

    @pl.when(owner)
    def _():
        with jax.named_scope("b_greet"):
            xs = [(x + d) % 4 * 16 for d in range(4)]
            zs = [(z + d) % 4 * 4 for d in range(4)]
            ys = [(y + d) % 4 for d in range(4)]
            for dx, dz, dy in FAR_FIRST:
                pl.semaphore_signal(
                    barrier, inc=1, device_id={"req": served, "seq": xs[dx] + zs[dz] + ys[dy]}, device_id_type=MESH)

            @pl.when(guest)
            def _():
                pl.semaphore_signal(barrier, inc=1, device_id={"req": 0, "seq": me}, device_id_type=MESH)

    @pl.when(home)
    def _():
        length_load.start()
        for source, target in text_slices:
            pltpu.make_async_copy(source, target, text_sem).start()

    @pl.when(feeder)
    def _():
        length_load.start()

    frequency, first, second, even = lanes()
    def settle(ref, sem):
        pltpu.make_async_copy(ref, ref, sem).wait()

    with jax.named_scope("c_loads"):
        loads[0].wait()
        settle(gains, gain_sem)
        settle(rows_in, rows_sem)
    with jax.named_scope("e_kv"):
        cosine, sine = rotary(order, frequency, first, second, even)
        for h in range(HEADS):
            cols = slice(h * HD, (h + 1) * HD)
            k = turn(ik[:, cols].astype(jnp.float32), gains[1:2, :], cosine, sine, even)
            v = iv[:, cols].astype(jnp.float32)
            kv_out[h] = jnp.concatenate([k, v], axis=0).astype(jnp.bfloat16)

    with jax.named_scope("f_barrier"):
        @pl.when(home)
        def _():
            pl.semaphore_wait(barrier, HEADS - 1)

        @pl.when(jnp.logical_not(home))
        def _():
            pl.semaphore_wait(barrier, HEADS)

    for h in range(HEADS):
        @pl.when(jnp.logical_or(request == 0, me != owners[h]))
        def _():
            pltpu.make_async_remote_copy(
                src_ref=kv_out.at[h], dst_ref=kv_in.at[spot], send_sem=send_sem, recv_sem=kv_recv,
                device_id={"req": 1, "seq": owners[h]}, device_id_type=MESH).start()

    for h in range(HEADS):
        cols = slice(h * HD, (h + 1) * HD)
        q = turn(iq[:, cols].astype(jnp.float32), gains[0:1, :], cosine, sine, even)
        q_out[h] = q.astype(jnp.bfloat16)
    for h in range(HEADS):
        @pl.when(jnp.logical_or(request == 0, me != owners[h]))
        def _():
            pltpu.make_async_remote_copy(
                src_ref=q_out.at[h], dst_ref=q_in.at[spot], send_sem=send_sem, recv_sem=q_recv.at[z // 2],
                device_id={"req": 1, "seq": owners[h]}, device_id_type=MESH).start()

    def feed(source, target, sem):
        return pltpu.make_async_remote_copy(
            src_ref=source, dst_ref=target, send_sem=sem, recv_sem=sem, device_id={"req": 1, "seq": me},
            device_id_type=MESH)

    @pl.when(feeder)
    def _():
        for source, target in text_slices:
            feed(source, target, text_sem).start()
        length_load.wait()
        length_out[...] = jnp.full(length_out.shape, length[0], jnp.int32)
        feed(length_out, length_in, length_sem).start()

    def drain(ref, count, sem):
        settle(ref.at[pl.ds(0, count)], sem)

    def arrived(ref, count, sem, own):
        @pl.when(own)
        def _():
            drain(ref, count - 1, sem)

        @pl.when(jnp.logical_not(own))
        def _():
            drain(ref, count, sem)

    def queries_arrived(pair):
        arrived(q_in, 2 * PLANE, q_recv.at[pair], jnp.logical_and(home, z // 2 == pair))

    @pl.when(owner)
    def _():
        @pl.when(home)
        def _():
            kv_in[spot] = kv_out[head]
            q_in[spot] = q_out[head]
            length_load.wait()
            length_in[...] = jnp.full(length_in.shape, length[0], jnp.int32)

        with jax.named_scope("j_feed"):
            settle(text_in, text_sem)

            @pl.when(guest)
            def _():
                settle(length_in, length_sem)

        with jax.named_scope("j_text"):
            text_keys = normed(tk[...].astype(jnp.float32), gains[3:4, :]).T.astype(jnp.bfloat16)
            text_values = tv[...]
            keys_in = lax.broadcasted_iota(jnp.int32, (1, text_keys.shape[1]), 1)
            valid = keys_in < across(length_in[0:1, :], keys_in)

            def text_part(q):
                s = jnp.where(valid, dot(q, text_keys), NEG)
                top = wide(jnp.max(s, axis=-1, keepdims=True))
                e = jnp.exp2((s - across(top, s)) * scale)
                total = wide(jnp.sum(e, axis=-1, keepdims=True))
                return top, total, dot(e.astype(jnp.bfloat16), text_values)

            half = PLANE * ROWS
            text_queries, text_state = {}, {}
            for group in range(4):
                rows = jnp.concatenate(
                    [tq[pl.ds(i * half + group * 32, 32), :] for i in range(4)], axis=0).astype(jnp.float32)
                text_queries[group] = normed(rows, gains[2:3, :]).astype(jnp.bfloat16)

        def both_parts(first, second):
            parts = text_part(jnp.concatenate([first, second], axis=0))
            return tuple(part[:half] for part in parts), tuple(part[half:] for part in parts)

        def image_queries(group):
            return q_in[pl.ds(group * PLANE, PLANE)].astype(jnp.float32).reshape(half, HD).astype(jnp.bfloat16)

        image_q, image_state = {}, {}
        with jax.named_scope("j_part"):
            for a, b in ((0, 1), (2, 3)):
                text_state[a], text_state[b] = both_parts(text_queries[a], text_queries[b])

        def image_part(a, b):
            for group in (a, b):
                image_q[group] = image_queries(group)
            image_state[a], image_state[b] = both_parts(image_q[a], image_q[b])

        with jax.named_scope("k_q"):
            queries_arrived(0)
        with jax.named_scope("k_text"):
            image_part(0, 1)
        with jax.named_scope("l_kv"):
            arrived(kv_in, SEQ, kv_recv, home)
        kv = kv_in[...].astype(jnp.float32)
        keys[...] = kv[:, :ROWS, :].reshape(SEQ * ROWS, HD).astype(jnp.bfloat16)
        values[...] = kv[:, ROWS:, :].reshape(SEQ * ROWS, HD).astype(jnp.bfloat16)
        for group in (0, 1, 2, 3):
            if group == 2:
                with jax.named_scope("l_q"):
                    queries_arrived(1)
                with jax.named_scope("m_text"):
                    image_part(2, 3)
            with jax.named_scope("n%d_image" % group):
                q = jnp.concatenate([image_q[group], text_queries[group]], axis=0)
                text_max, text_sum, text_out = (
                    jnp.concatenate(part, axis=0) for part in zip(image_state[group], text_state[group]))
                s = lax.dot_general(
                    q, keys[...], (((1,), (1,)), ((), ())), preferred_element_type=jnp.float32)
                top = jnp.maximum(wide(jnp.max(s, axis=-1, keepdims=True)), text_max)
                e = jnp.exp2((s - across(top, s)) * scale)
                keep = jnp.exp2((text_max - top) * scale)
                total = wide(jnp.sum(e, axis=-1, keepdims=True)) + text_sum * keep
                o = dot(e.astype(jnp.bfloat16), values[...]) + text_out * keep
                o = o / total
                image, text = o[:half].reshape(PLANE, ROWS, HD), o[half:].reshape(PLANE, ROWS, HD)
                o_out[pl.ds(group * PLANE, PLANE)] = jnp.concatenate([image, text], axis=1).astype(jnp.bfloat16)
            with jax.named_scope("n%d_send" % group):
                for i in (0, 12, 8, 4, 1, 13, 3, 15, 9, 11, 5, 7, 2, 14, 10, 6):
                    to = at(i // 4, group, i % 4)

                    def send():
                        pltpu.make_async_remote_copy(
                            src_ref=o_out.at[group * PLANE + i], dst_ref=o_in.at[head], send_sem=o_send,
                            recv_sem=o_recv, device_id={"req": served, "seq": to}, device_id_type=MESH).start()

                    if to in HOME:
                        pl.when(jnp.logical_or(guest, me != to))(send)
                    else:
                        send()
        @pl.when(home)
        def _():
            o_in[head] = o_out[spot]
            drain(o_out, SEQ - 1, o_send)

        @pl.when(guest)
        def _():
            drain(o_out, SEQ, o_send)

    @pl.when(feeder)
    def _():
        settle(text_in, text_sem)
        settle(length_out, length_sem)

    @pl.when(home)
    def _():
        drain(q_in, 3 * (HEADS - 1), send_sem)
        with jax.named_scope("o_wait"):
            drain(o_in, HEADS - 1, o_recv)

    @pl.when(jnp.logical_not(home))
    def _():
        drain(q_in, 3 * HEADS, send_sem)
        with jax.named_scope("p_wait"):
            drain(o_in, HEADS, o_recv)


def spread(o_in, image_hbm, text_hbm, image, text, sem):
    for block, block_hbm, rows in ((image, image_hbm, slice(0, ROWS)), (text, text_hbm, slice(ROWS, 2 * ROWS))):
        for h in range(HEADS):
            block[:, h * HD:(h + 1) * HD] = o_in[h].astype(jnp.float32)[rows].astype(jnp.bfloat16)
        pltpu.make_async_copy(block, block_hbm, sem).start()
    pltpu.make_async_copy(o_in, o_in, sem).wait()


def local(image_query, image_key, image_value, text_query, text_key, text_value, image_query_gain,
          image_key_gain, text_query_gain, text_key_gain, image_order, text_length):
    hbm = pl.BlockSpec(memory_space=pl.ANY)
    vmem = pl.BlockSpec(memory_space=pltpu.VMEM)
    bf16, f32 = jnp.bfloat16, jnp.float32
    width = image_query.shape[1]
    text_rows = text_key.shape[0]
    dma = pltpu.SemaphoreType.DMA
    gains = [g.reshape(1, HD) for g in (image_query_gain, image_key_gain, text_query_gain, text_key_gain)]
    blocks = pl.pallas_call(
        kernel,
        out_shape=pltpu.VMEM((HEADS, 2 * ROWS, HD), bf16),
        in_specs=[hbm] * 12,
        out_specs=vmem,
        scratch_shapes=[
            pltpu.SMEM((ROWS,), jnp.int32),
            pltpu.SMEM((1,), jnp.int32),
            pltpu.VMEM((3, ROWS, width), bf16),
            pltpu.VMEM((3, text_rows, HD), bf16),
            pltpu.VMEM((4, HD), f32),
            pltpu.VMEM((HEADS, 2 * ROWS, HD), bf16),
            pltpu.VMEM((HEADS, ROWS, HD), bf16),
            pltpu.VMEM((SEQ, 2 * ROWS, HD), bf16),
            pltpu.VMEM((SEQ, ROWS, HD), bf16),
            pltpu.VMEM((SEQ * ROWS, HD), bf16),
            pltpu.VMEM((SEQ * ROWS, HD), bf16),
            pltpu.VMEM((SEQ, 2 * ROWS, HD), bf16),
            pltpu.VMEM((ROWS, HD), jnp.int32),
            pltpu.VMEM((ROWS, HD), jnp.int32),
            dma, dma, dma, dma, dma, dma, dma, dma((2,)), dma, dma,
        ],
        compiler_params=pltpu.CompilerParams(collective_id=0, has_side_effects=True),
        name="joint",
    )(image_order, text_length, image_query, image_key, image_value, text_query, text_key, text_value, *gains)
    out = jax.ShapeDtypeStruct((ROWS, width), bf16)
    return pl.pallas_call(
        spread,
        out_shape=(out, out),
        in_specs=[vmem],
        out_specs=(hbm, hbm),
        scratch_shapes=[pltpu.VMEM((ROWS, width), bf16), pltpu.VMEM((ROWS, width), bf16), dma],
        name="spread",
    )(pltpu.with_memory_space_constraint(blocks, pltpu.VMEM))


def solution(mesh):
    placed = (
        P(("req", "seq"), None),
        P(("req", "seq"), None),
        P(("req", "seq"), None),
        P("req", None),
        P("req", None),
        P("req", None),
        P(),
        P(),
        P(),
        P(),
        P(("req", "seq")),
        P("req"),
    )
    return jax.shard_map(
        local,
        mesh=mesh,
        in_specs=placed,
        out_specs=(P(("req", "seq"), None), P(("req", "seq"), None)),
        check_vma=False,
    )
```

```python
import jax
import jax.numpy as jnp
from jax import lax
from jax.experimental import pallas as pl
from jax.experimental.pallas import tpu as pltpu
from jax.sharding import PartitionSpec as P

GRID_W = 64
EPS = 1e-06
NEG = -1e30
MESH = pl.DeviceIdType.MESH
HEADS = 12
HD = 128
ROWS = 8
PLANE = 16
SEQ = 64
LOG2E = 1.4426950408889634


def at(x, z, y):
    return x * 16 + z * 4 + y


OWNERS = (
    [at(0, 0, 0), at(1, 0, 0), at(0, 0, 1), at(0, 1, 0), at(3, 0, 0), at(1, 0, 1),
     at(0, 0, 2), at(2, 0, 0), at(1, 1, 0), at(2, 0, 1), at(0, 1, 1), at(0, 0, 3)],
    [at(3, 0, 1), at(1, 0, 2), at(1, 2, 0), at(2, 1, 0), at(3, 1, 1), at(3, 1, 0),
     at(0, 1, 2), at(1, 1, 1), at(0, 1, 3), at(1, 1, 3), at(0, 2, 0), at(0, 3, 0)],
)
HOME = set(OWNERS[1])


def ring(a):
    return min(a, 4 - a)


FAR_FIRST = sorted([(t // 16, t // 4 % 4, t % 4) for t in range(1, SEQ)], key=lambda d: -sum(map(ring, d)))


def normed(x, gain):
    mean_square = jnp.mean(x * x, axis=-1, keepdims=True)
    return x * lax.rsqrt(mean_square + EPS) * gain


def lanes():
    lane = lax.broadcasted_iota(jnp.int32, (ROWS, HD), 1)
    pair = lane >> 1
    first = pair < 8
    second = pair < 36
    within = jnp.where(first, pair, jnp.where(second, pair - 8, pair - 36)).astype(jnp.float32)
    width = jnp.where(first, 16.0, 56.0).astype(jnp.float32)
    frequency = jnp.exp(within / width * jnp.float32(-2.0 * 9.210340371976184))
    return frequency, first, second, (lane & 1) == 0


def rotary(order_ref, frequency, first, second, even):
    row = lax.broadcasted_iota(jnp.int32, (ROWS, HD), 0)
    position = jnp.zeros((ROWS, HD), jnp.int32)
    for r in range(ROWS):
        position = jnp.where(row == r, order_ref[r], position)
    half = 4 * GRID_W
    inside = position & (half - 1)
    place = jnp.where(first, position >> 8, jnp.where(second, inside >> 6, inside & (GRID_W - 1)))
    angle = place.astype(jnp.float32) * frequency
    sine = jnp.sin(angle)
    return jnp.cos(angle), jnp.where(even, -sine, sine)


def swap(x, even):
    return jnp.where(even, pltpu.roll(x, HD - 1, 1), pltpu.roll(x, 1, 1))


def turn(x, gain, cosine, sine, even):
    gains = jnp.broadcast_to(gain, x.shape)
    same, other = gains * cosine, swap(gains, even) * sine
    scale = lax.rsqrt(jnp.mean(x * x, axis=-1, keepdims=True) + EPS)
    return (x * same + swap(x, even) * other) * scale


def wide(column):
    return jnp.broadcast_to(column, (column.shape[0], HD))


def across(block, like):
    return jnp.concatenate([block] * (like.shape[1] // HD), axis=1)


def dot(a, b):
    return jnp.dot(a, b, preferred_element_type=jnp.float32)


def kernel(order_hbm, length_hbm, iq_hbm, ik_hbm, iv_hbm, tq_hbm, tk_hbm, tv_hbm,
           iq_gain_hbm, ik_gain_hbm, tq_gain_hbm, tk_gain_hbm,
           o_in,
           order, length, rows_in, text_in, gains, kv_out, q_out, kv_in, q_in, keys, values, o_out, length_out, length_in,
           order_sem, rows_sem, gain_sem, text_sem, length_sem, send_sem, kv_recv, q_recv, o_send, o_recv):
    ik, iv, iq = rows_in.at[0], rows_in.at[1], rows_in.at[2]
    tk, tv, tq = text_in.at[0], text_in.at[1], text_in.at[2]
    loads = [pltpu.make_async_copy(order_hbm, order, order_sem)]
    loads += [pltpu.make_async_copy(a, b, rows_sem) for a, b in ((ik_hbm, ik), (iv_hbm, iv), (iq_hbm, iq))]
    loads += [
        pltpu.make_async_copy(a, gains.at[i:i + 1], gain_sem)
        for i, a in enumerate((iq_gain_hbm, ik_gain_hbm, tq_gain_hbm, tk_gain_hbm))]
    for load in loads:
        load.start()
    me, request = lax.axis_index("seq"), lax.axis_index("req")
    x, z, y = me // 16, (me // 4) % 4, me % 4
    spot = z * 16 + x * 4 + y
    owners = [jnp.where(request == 1, b, a) for a, b in zip(*OWNERS)]
    head = jnp.int32(0)
    chip_first = me == OWNERS[0][0]
    chip_second = me == OWNERS[1][0]
    for h in range(1, HEADS):
        first, second = me == OWNERS[0][h], me == OWNERS[1][h]
        head = jnp.where(jnp.logical_or(first, second), h, head)
        chip_first, chip_second = jnp.logical_or(chip_first, first), jnp.logical_or(chip_second, second)
    feeder = jnp.logical_and(request == 0, chip_first)
    guest = jnp.logical_and(request == 1, chip_first)
    home = jnp.logical_and(request == 1, chip_second)
    owner = jnp.logical_or(guest, home)
    served = jnp.where(guest, 0, 1)
    scale = HD ** -0.5 * LOG2E

    barrier = pltpu.get_barrier_semaphore()
    column = pl.ds(pl.multiple_of(head * HD, HD), HD)
    length_load = pltpu.make_async_copy(length_hbm, length, length_sem)
    text_slices = [(tk_hbm.at[:, column], tk), (tv_hbm.at[:, column], tv), (tq_hbm.at[:, column], tq)]

    @pl.when(owner)
    def _():
        with jax.named_scope("b_greet"):
            xs = [(x + d) % 4 * 16 for d in range(4)]
            zs = [(z + d) % 4 * 4 for d in range(4)]
            ys = [(y + d) % 4 for d in range(4)]
            for dx, dz, dy in FAR_FIRST:
                pl.semaphore_signal(
                    barrier, inc=1, device_id={"req": served, "seq": xs[dx] + zs[dz] + ys[dy]}, device_id_type=MESH)

            @pl.when(guest)
            def _():
                pl.semaphore_signal(barrier, inc=1, device_id={"req": 0, "seq": me}, device_id_type=MESH)

    @pl.when(home)
    def _():
        length_load.start()
        for source, target in text_slices:
            pltpu.make_async_copy(source, target, text_sem).start()

    @pl.when(feeder)
    def _():
        length_load.start()

    frequency, first, second, even = lanes()
    def settle(ref, sem):
        pltpu.make_async_copy(ref, ref, sem).wait()

    with jax.named_scope("c_loads"):
        loads[0].wait()
        settle(gains, gain_sem)
        settle(rows_in, rows_sem)
    with jax.named_scope("e_kv"):
        cosine, sine = rotary(order, frequency, first, second, even)
        for h in range(HEADS):
            cols = slice(h * HD, (h + 1) * HD)
            k = turn(ik[:, cols].astype(jnp.float32), gains[1:2, :], cosine, sine, even)
            v = iv[:, cols].astype(jnp.float32)
            kv_out[h] = jnp.concatenate([k, v], axis=0).astype(jnp.bfloat16)

    with jax.named_scope("f_barrier"):
        @pl.when(home)
        def _():
            pl.semaphore_wait(barrier, HEADS - 1)

        @pl.when(jnp.logical_not(home))
        def _():
            pl.semaphore_wait(barrier, HEADS)

    for h in range(HEADS):
        @pl.when(jnp.logical_or(request == 0, me != owners[h]))
        def _():
            pltpu.make_async_remote_copy(
                src_ref=kv_out.at[h], dst_ref=kv_in.at[spot], send_sem=send_sem, recv_sem=kv_recv,
                device_id={"req": 1, "seq": owners[h]}, device_id_type=MESH).start()

    for h in range(HEADS):
        cols = slice(h * HD, (h + 1) * HD)
        q = turn(iq[:, cols].astype(jnp.float32), gains[0:1, :], cosine, sine, even)
        q_out[h] = q.astype(jnp.bfloat16)
    for h in range(HEADS):
        @pl.when(jnp.logical_or(request == 0, me != owners[h]))
        def _():
            pltpu.make_async_remote_copy(
                src_ref=q_out.at[h], dst_ref=q_in.at[spot], send_sem=send_sem, recv_sem=q_recv.at[z // 2],
                device_id={"req": 1, "seq": owners[h]}, device_id_type=MESH).start()

    def feed(source, target, sem):
        return pltpu.make_async_remote_copy(
            src_ref=source, dst_ref=target, send_sem=sem, recv_sem=sem, device_id={"req": 1, "seq": me},
            device_id_type=MESH)

    @pl.when(feeder)
    def _():
        for source, target in text_slices:
            feed(source, target, text_sem).start()
        length_load.wait()
        length_out[...] = jnp.full(length_out.shape, length[0], jnp.int32)
        feed(length_out, length_in, length_sem).start()

    def drain(ref, count, sem):
        settle(ref.at[pl.ds(0, count)], sem)

    def arrived(ref, count, sem, own):
        @pl.when(own)
        def _():
            drain(ref, count - 1, sem)

        @pl.when(jnp.logical_not(own))
        def _():
            drain(ref, count, sem)

    def queries_arrived(pair):
        arrived(q_in, 2 * PLANE, q_recv.at[pair], jnp.logical_and(home, z // 2 == pair))

    @pl.when(owner)
    def _():
        @pl.when(home)
        def _():
            kv_in[spot] = kv_out[head]
            q_in[spot] = q_out[head]
            length_load.wait()
            length_in[...] = jnp.full(length_in.shape, length[0], jnp.int32)

        with jax.named_scope("j_feed"):
            settle(text_in, text_sem)

            @pl.when(guest)
            def _():
                settle(length_in, length_sem)

        with jax.named_scope("j_text"):
            text_keys = normed(tk[...].astype(jnp.float32), gains[3:4, :]).T.astype(jnp.bfloat16)
            text_values = tv[...]
            keys_in = lax.broadcasted_iota(jnp.int32, (1, text_keys.shape[1]), 1)
            valid = keys_in < across(length_in[0:1, :], keys_in)

            def text_part(q):
                s = jnp.where(valid, dot(q, text_keys), NEG)
                top = wide(jnp.max(s, axis=-1, keepdims=True))
                e = jnp.exp2((s - across(top, s)) * scale)
                total = wide(jnp.sum(e, axis=-1, keepdims=True))
                return top, total, dot(e.astype(jnp.bfloat16), text_values)

            half = PLANE * ROWS
            text_queries, text_state = {}, {}
            for group in range(4):
                rows = jnp.concatenate(
                    [tq[pl.ds(i * half + group * 32, 32), :] for i in range(4)], axis=0).astype(jnp.float32)
                text_queries[group] = normed(rows, gains[2:3, :]).astype(jnp.bfloat16)

        def both_parts(first, second):
            parts = text_part(jnp.concatenate([first, second], axis=0))
            return tuple(part[:half] for part in parts), tuple(part[half:] for part in parts)

        def image_queries(group):
            return q_in[pl.ds(group * PLANE, PLANE)].astype(jnp.float32).reshape(half, HD).astype(jnp.bfloat16)

        image_q, image_state = {}, {}
        with jax.named_scope("j_part"):
            for a, b in ((0, 1), (2, 3)):
                text_state[a], text_state[b] = both_parts(text_queries[a], text_queries[b])

        def image_part(a, b):
            for group in (a, b):
                image_q[group] = image_queries(group)
            image_state[a], image_state[b] = both_parts(image_q[a], image_q[b])

        with jax.named_scope("k_q"):
            queries_arrived(0)
        with jax.named_scope("k_text"):
            image_part(0, 1)
        with jax.named_scope("l_kv"):
            arrived(kv_in, SEQ, kv_recv, home)
        kv = kv_in[...].astype(jnp.float32)
        keys[...] = kv[:, :ROWS, :].reshape(SEQ * ROWS, HD).astype(jnp.bfloat16)
        values[...] = kv[:, ROWS:, :].reshape(SEQ * ROWS, HD).astype(jnp.bfloat16)
        for group in (0, 1, 2, 3):
            if group == 2:
                with jax.named_scope("l_q"):
                    queries_arrived(1)
                with jax.named_scope("m_text"):
                    image_part(2, 3)
            with jax.named_scope("n%d_image" % group):
                q = jnp.concatenate([image_q[group], text_queries[group]], axis=0)
                text_max, text_sum, text_out = (
                    jnp.concatenate(part, axis=0) for part in zip(image_state[group], text_state[group]))
                s = lax.dot_general(
                    q, keys[...], (((1,), (1,)), ((), ())), preferred_element_type=jnp.float32)
                top = jnp.maximum(wide(jnp.max(s, axis=-1, keepdims=True)), text_max)
                e = jnp.exp2((s - across(top, s)) * scale)
                keep = jnp.exp2((text_max - top) * scale)
                total = wide(jnp.sum(e, axis=-1, keepdims=True)) + text_sum * keep
                o = dot(e.astype(jnp.bfloat16), values[...]) + text_out * keep
                o = o / total
                image, text = o[:half].reshape(PLANE, ROWS, HD), o[half:].reshape(PLANE, ROWS, HD)
                o_out[pl.ds(group * PLANE, PLANE)] = jnp.concatenate([image, text], axis=1).astype(jnp.bfloat16)
            with jax.named_scope("n%d_send" % group):
                for i in (0, 12, 8, 4, 1, 13, 3, 15, 9, 11, 5, 7, 2, 14, 10, 6):
                    to = at(i // 4, group, i % 4)

                    def send():
                        pltpu.make_async_remote_copy(
                            src_ref=o_out.at[group * PLANE + i], dst_ref=o_in.at[head], send_sem=o_send,
                            recv_sem=o_recv, device_id={"req": served, "seq": to}, device_id_type=MESH).start()

                    if to in HOME:
                        pl.when(jnp.logical_or(guest, me != to))(send)
                    else:
                        send()
        @pl.when(home)
        def _():
            o_in[head] = o_out[spot]
            drain(o_out, SEQ - 1, o_send)

        @pl.when(guest)
        def _():
            drain(o_out, SEQ, o_send)

    @pl.when(feeder)
    def _():
        settle(text_in, text_sem)
        settle(length_out, length_sem)

    @pl.when(home)
    def _():
        drain(q_in, 3 * (HEADS - 1), send_sem)
        with jax.named_scope("o_wait"):
            drain(o_in, HEADS - 1, o_recv)

    @pl.when(jnp.logical_not(home))
    def _():
        drain(q_in, 3 * HEADS, send_sem)
        with jax.named_scope("p_wait"):
            drain(o_in, HEADS, o_recv)


def spread(o_in, image_hbm, text_hbm, image, text, sem):
    for block, block_hbm, rows in ((image, image_hbm, slice(0, ROWS)), (text, text_hbm, slice(ROWS, 2 * ROWS))):
        for h in range(HEADS):
            block[:, h * HD:(h + 1) * HD] = o_in[h].astype(jnp.float32)[rows].astype(jnp.bfloat16)
        pltpu.make_async_copy(block, block_hbm, sem).start()
    pltpu.make_async_copy(o_in, o_in, sem).wait()


def local(image_query, image_key, image_value, text_query, text_key, text_value, image_query_gain,
          image_key_gain, text_query_gain, text_key_gain, image_order, text_length):
    hbm = pl.BlockSpec(memory_space=pl.ANY)
    vmem = pl.BlockSpec(memory_space=pltpu.VMEM)
    bf16, f32 = jnp.bfloat16, jnp.float32
    width = image_query.shape[1]
    text_rows = text_key.shape[0]
    dma = pltpu.SemaphoreType.DMA
    gains = [g.reshape(1, HD) for g in (image_query_gain, image_key_gain, text_query_gain, text_key_gain)]
    blocks = pl.pallas_call(
        kernel,
        out_shape=pltpu.VMEM((HEADS, 2 * ROWS, HD), bf16),
        in_specs=[hbm] * 12,
        out_specs=vmem,
        scratch_shapes=[
            pltpu.SMEM((ROWS,), jnp.int32),
            pltpu.SMEM((1,), jnp.int32),
            pltpu.VMEM((3, ROWS, width), bf16),
            pltpu.VMEM((3, text_rows, HD), bf16),
            pltpu.VMEM((4, HD), f32),
            pltpu.VMEM((HEADS, 2 * ROWS, HD), bf16),
            pltpu.VMEM((HEADS, ROWS, HD), bf16),
            pltpu.VMEM((SEQ, 2 * ROWS, HD), bf16),
            pltpu.VMEM((SEQ, ROWS, HD), bf16),
            pltpu.VMEM((SEQ * ROWS, HD), bf16),
            pltpu.VMEM((SEQ * ROWS, HD), bf16),
            pltpu.VMEM((SEQ, 2 * ROWS, HD), bf16),
            pltpu.VMEM((ROWS, HD), jnp.int32),
            pltpu.VMEM((ROWS, HD), jnp.int32),
            dma, dma, dma, dma, dma, dma, dma, dma((2,)), dma, dma,
        ],
        compiler_params=pltpu.CompilerParams(collective_id=0, has_side_effects=True),
        name="joint",
    )(image_order, text_length, image_query, image_key, image_value, text_query, text_key, text_value, *gains)
    out = jax.ShapeDtypeStruct((ROWS, width), bf16)
    return pl.pallas_call(
        spread,
        out_shape=(out, out),
        in_specs=[vmem],
        out_specs=(hbm, hbm),
        scratch_shapes=[pltpu.VMEM((ROWS, width), bf16), pltpu.VMEM((ROWS, width), bf16), dma],
        name="spread",
    )(pltpu.with_memory_space_constraint(blocks, pltpu.VMEM))


def solution(mesh):
    placed = (
        P(("req", "seq"), None),
        P(("req", "seq"), None),
        P(("req", "seq"), None),
        P("req", None),
        P("req", None),
        P("req", None),
        P(),
        P(),
        P(),
        P(),
        P(("req", "seq")),
        P("req"),
    )
    return jax.shard_map(
        local,
        mesh=mesh,
        in_specs=placed,
        out_specs=(P(("req", "seq"), None), P(("req", "seq"), None)),
        check_vma=False,
    )
```
